256 devices in a mesh: tm: 4 (over y), sx: 8 (over x, core), sy: 8 (over z).
Axes of the slice: x: 4, y: 4, z: 8, core: 2. Of those that a mesh axis runs over, the one named last changes fastest.
Arguments:
- iterate: float32 [32, 2048, 2048], P('tm', 'sx', 'sy'), may hold values from -6 to 6
- source: float32 [32, 2048, 2048], P('tm', 'sx', 'sy'), may hold values from -6 to 6
- start_field: float32 [2048, 2048], P('sx', 'sy'), may hold values from -6 to 6
- conduct: float32 [2048, 2048], P('sx', 'sy'), may hold values from 0.2 to 5
Outputs:
- updated: float32 [32, 2048, 2048], P('tm', 'sx', 'sy')
- coarse_residual: float32 [8, 2048, 2048], P('tm', 'sx', 'sy')
The draws below stay inside these ranges and needn't reach their ends.
All inputs are finite; a program needn't handle non-finite values.
Results may differ from the reference program's by a relative error of at most 0.00002.
Values sent between devices are 32-bit elements; how exact they have to be, the bound alone decides.
No kernel may reach another device: no remote copies, remote signals or barrier semaphores. Data moves between devices by JAX's collectives and lax.ppermute only.
A program may use at most 128 MiB of HBM per device.

```python
import math
import jax
import jax.numpy as jnp

FACTOR = 4
SWEEPS = 2
NT = 32
NX = 2048
NY = 2048


def steps_of(own_key, shape, split, low, top_value):
    def one(position, blocks):
        heights = jax.random.uniform(jax.random.fold_in(jax.random.fold_in(own_key, 6), position), (blocks,), jnp.float32, low / len(split), top_value / len(split))
        return jnp.repeat(jnp.exp(heights), shape[position] // blocks).reshape((-1,) + (1,) * (len(shape) - position - 1))

    level = one(*split[0])
    for cut in split[1:]:
        level = level * one(*cut)
    return level


def bell_draw(stream_key, shape, scale, bound, split=(), dtype=jnp.bfloat16):
    result = jax.random.normal(stream_key, shape, jnp.float32) * scale
    if len(split) > 0:
        result = steps_of(stream_key, shape, split, -0.22, 0.18) * result
    return jnp.clip(result, min=-bound, max=bound).astype(dtype)


def setup_inputs(seed: int = 0) -> dict:
    key_of = jax.random.split(jax.random.key(seed), 5)
    iterate = bell_draw(key_of[0], (NT, NX, NY), 1.0, 6.0, ((0, 4), (1, 8), (2, 8)), jnp.float32)
    source = bell_draw(key_of[1], (NT, NX, NY), 1.0, 6.0, ((0, 4), (1, 8), (2, 8)), jnp.float32)
    start_field = bell_draw(key_of[2], (NX, NY), 1.0, 6.0, ((0, 8), (1, 8)), jnp.float32)
    conduct = jnp.clip(jnp.exp(math.log(5.0) - 3.218876 * jax.random.uniform(key_of[3], (NX, NY), jnp.float32) ** steps_of(key_of[3], (NX, NY), ((0, 8), (1, 8)), -0.2, 0.2)), 0.2, 5.0)
    return {"iterate": iterate, "source": source, "start_field": start_field, "conduct": conduct}


def neighbours(padded):
    total = padded[:, 2:, 1:-1] + padded[:, :-2, 1:-1]
    return total + padded[:, 1:-1, 2:] + padded[:, 1:-1, :-2]


def implicit_step(rhs, coeff):
    denom = 1.0 + 4.0 * coeff
    field = rhs
    for sweep in range(SWEEPS):
        padded = jnp.pad(field, ((0, 0), (1, 1), (1, 1)))
        field = (rhs + coeff * neighbours(padded)) / denom
    return field


def restrict(field):
    shape = field.shape
    blocks = field.reshape(shape[0], shape[1] // 2, 2, shape[2] // 2, 2)
    return 0.25 * jnp.sum(blocks, axis=(2, 4))


def prolong(field):
    return jnp.repeat(jnp.repeat(field, 2, axis=1), 2, axis=2)


def reference(iterate, source, start_field, conduct):
    count = NT // FACTOR
    state = iterate.reshape(count, FACTOR, NX, NY)
    forcing = source.reshape(count, FACTOR, NX, NY)

    def relax_fine(state):
        field = jnp.concatenate([start_field[None], state[:-1, FACTOR - 1]], axis=0)
        columns = []
        for place in range(FACTOR - 1):
            field = implicit_step(field + forcing[:, place], conduct)
            columns.append(field)
        columns.append(state[:, FACTOR - 1])
        return jnp.stack(columns, axis=1)

    def relax_coarse(state):
        point = implicit_step(state[:, FACTOR - 2] + forcing[:, FACTOR - 1], conduct)
        return state.at[:, FACTOR - 1].set(point)

    state = relax_fine(state)
    state = relax_coarse(state)
    state = relax_fine(state)
    resid = implicit_step(state[:, FACTOR - 2] + forcing[:, FACTOR - 1], conduct) - state[:, FACTOR - 1]
    coarse_rhs = restrict(resid)
    coarse_coeff = restrict(conduct[None])[0]
    error = jnp.zeros((1, NX // 2, NY // 2), jnp.float32)
    errors = []
    for level in range(count):
        error = implicit_step(error, coarse_coeff) + coarse_rhs[level][None]
        errors.append(error[0])
    correction = prolong(jnp.stack(errors, axis=0))
    state = state.at[:, FACTOR - 1].add(correction)
    state = relax_fine(state)
    return state.reshape(NT, NX, NY), resid
```

```python
import functools

import jax
import jax.numpy as jnp
from jax import lax
from jax.experimental import pallas as pl
from jax.experimental.pallas import tpu as pltpu
from jax.sharding import PartitionSpec as P

FACTOR = 4
N = 256
HALO = 16
PAD = 8
EXT = N + 2 * HALO
ROWS = EXT + 2 * PAD
TOP = PAD + HALO
C = N // 2
CEXT = C + 2 * HALO
CROWS = CEXT + 2 * PAD
FIELDS = 11
MID, LAST, COEF = 8, 9, 10
F32 = jnp.float32
LIMIT = 24 * 1024 * 1024

VM = pl.BlockSpec(memory_space=pltpu.VMEM)


def call(body, outs, n_in, scratch=(), aliases=None, name=None, flops=0):
    return pl.pallas_call(
        body,
        out_shape=[jax.ShapeDtypeStruct(s, F32) for s in outs],
        in_specs=[VM] * n_in,
        out_specs=[VM] * len(outs),
        scratch_shapes=list(scratch),
        input_output_aliases=aliases or {},
        name=name,
        compiler_params=pltpu.CompilerParams(vmem_limit_bytes=LIMIT),
        cost_estimate=pl.CostEstimate(flops=flops, bytes_accessed=1000, transcendentals=0),
    )


def lanes(rows):
    return lax.broadcasted_iota(jnp.int32, (rows, 128), 1)


def roll(x, by):
    by %= 128
    return pltpu.roll(x, by, 1) if by else x


def stencil(ref, f, base, rows, cols, first, last):
    mid = [ref[f, j, pl.ds(base, rows), :] for j in range(cols)]
    left = [pltpu.roll(m, 1, 1) for m in mid]
    right = [pltpu.roll(m, 127, 1) for m in mid]
    sums = []
    for j in range(cols):
        total = ref[f, j, pl.ds(base + 1, rows), :] + ref[f, j, pl.ds(base - 1, rows), :]
        side = jnp.where(first, left[j - 1], left[j]) + jnp.where(last, right[(j + 1) % cols], right[j])
        sums.append(total + side)
    return mid, sums


def loop(total, rows, body):
    def step(i, carry):
        body(PAD + pl.multiple_of(i * rows, 8))
        return carry

    lax.fori_loop(0, total // rows, step, 0)


def step(rhs, mid, scaled, inv, cof, fields, cols, total, rows, after):
    def one(base):
        lane = lanes(rows)
        first, last = lane == 0, lane == 127
        for f in fields:
            own, sums = stencil(rhs, f, base, rows, cols, first, last)
            for j in range(cols):
                at = (j, pl.ds(base, rows), slice(None))
                b = own[j] * inv[at]
                scaled[(f, *at)] = b
                mid[(f, *at)] = b + cof[at] * sums[j]

    def two(base):
        lane = lanes(rows)
        first, last = lane == 0, lane == 127
        for f in fields:
            _, sums = stencil(mid, f, base, rows, cols, first, last)
            for j in range(cols):
                at = (j, pl.ds(base, rows), slice(None))
                u = scaled[(f, *at)] + cof[at] * sums[j]
                rhs[(f, *at)] = after(f, j, pl.ds(base, rows), u)

    loop(total, rows, one)
    loop(total, rows, two)


def keep(f, j, at, u):
    return u


def clear_pads(refs, fields, cols, total):
    zero = jnp.zeros((PAD, 128), F32)
    for ref in refs:
        for f in range(fields):
            for j in range(cols):
                ref[f, j, 0:PAD, :] = zero
                ref[f, j, PAD + total : 2 * PAD + total, :] = zero


def restrict(ref, f, base):
    fine = lax.broadcasted_iota(jnp.int32, (128, C), 0) // 2
    coarse = lax.broadcasted_iota(jnp.int32, (128, C), 1)
    out = None
    for j in range(2):
        pair = ref[f, j, pl.ds(base, C, stride=2), :] + ref[f, j, pl.ds(base + 1, C, stride=2), :]
        pick = jnp.where(fine + 64 * j == coarse, 0.25, 0.0).astype(F32)
        part = jnp.dot(pair, pick, precision=lax.Precision.HIGHEST, preferred_element_type=F32)
        out = part if out is None else out + part
    return out


def flag(condition):
    return jnp.where(condition, 1.0, 0.0).astype(F32)


def strips_body(s_top, s_bot, m_top, m_bot, l_all, start, c_top, c_bot, up, down, last):
    is_end = lax.axis_index("tm") == lax.axis_size("tm") - 1
    up[0:8] = s_top[...]
    down[0:8] = s_bot[...]
    up[MID] = m_top[0]
    down[MID] = m_bot[0]
    up[COEF] = c_top[...]
    down[COEF] = c_bot[...]

    @pl.when(is_end)
    def _():
        last[...] = start[...]

    @pl.when(jnp.logical_not(is_end))
    def _():
        last[...] = l_all[0]

    up[LAST] = last[0:HALO, :]
    down[LAST] = last[N - HALO : N, :]


def make_strips(iterate, source, start, conduct):
    hi = N // HALO - 1
    return pl.pallas_call(
        strips_body,
        grid=(1,),
        out_shape=[
            jax.ShapeDtypeStruct((FIELDS, HALO, N), F32),
            jax.ShapeDtypeStruct((FIELDS, HALO, N), F32),
            jax.ShapeDtypeStruct((N, N), F32),
        ],
        in_specs=[
            pl.BlockSpec((8, HALO, N), lambda i: (0, 0, 0)),
            pl.BlockSpec((8, HALO, N), lambda i: (0, hi, 0)),
            pl.BlockSpec((1, HALO, N), lambda i: (3, 0, 0)),
            pl.BlockSpec((1, HALO, N), lambda i: (3, hi, 0)),
            pl.BlockSpec((1, N, N), lambda i: (7, 0, 0)),
            pl.BlockSpec((N, N), lambda i: (0, 0)),
            pl.BlockSpec((HALO, N), lambda i: (0, 0)),
            pl.BlockSpec((HALO, N), lambda i: (hi, 0)),
        ],
        out_specs=[
            pl.BlockSpec((FIELDS, HALO, N), lambda i: (0, 0, 0)),
            pl.BlockSpec((FIELDS, HALO, N), lambda i: (0, 0, 0)),
            pl.BlockSpec((N, N), lambda i: (0, 0)),
        ],
        name="strips",
        compiler_params=pltpu.CompilerParams(vmem_limit_bytes=LIMIT),
    )(source, source, iterate, iterate, iterate, start, conduct, conduct)


def pack_edges(pieces, rows):
    lane = lanes(rows)
    low = [jnp.zeros((rows, 128), F32) for _ in range((len(pieces) + 7) // 8)]
    high = list(low)
    for f, (head, tail) in enumerate(pieces):
        at, k = HALO * (f % 8), f // 8
        inside = (lane >= at) & (lane < at + HALO)
        low[k] = jnp.where(inside, roll(head, at), low[k])
        high[k] = jnp.where(inside, roll(tail, at + HALO), high[k])
    return low, high


def center_body(source, middle, last, conduct, ext, low, high):
    rows = 16

    def chunk(i, carry):
        base = pl.multiple_of(i * rows, 8)
        pieces = []
        for f in range(FIELDS):
            at = (pl.ds(base, rows), slice(None))
            x = source[(f, *at)] if f < 8 else middle[(0, *at)] if f == MID else last[at] if f == LAST else conduct[at]
            head, tail = x[:, :128], x[:, 128:]
            ext[f, 0, pl.ds(TOP + base, rows), :] = head
            ext[f, 1, pl.ds(TOP + base, rows), :] = tail
            pieces.append((head, tail))
        lo, hi = pack_edges(pieces, rows)
        for k in range(2):
            low[pl.ds(base, rows), 128 * k : 128 * k + 128] = lo[k]
            high[pl.ds(base, rows), 128 * k : 128 * k + 128] = hi[k]
        return carry

    lax.fori_loop(0, N // rows, chunk, 0)


def make_center(source, iterate, last, conduct):
    return pl.pallas_call(
        center_body,
        grid=(1,),
        out_shape=[
            jax.ShapeDtypeStruct((FIELDS, 3, ROWS, 128), F32),
            jax.ShapeDtypeStruct((N, 256), F32),
            jax.ShapeDtypeStruct((N, 256), F32),
        ],
        in_specs=[
            VM,
            pl.BlockSpec((1, N, N), lambda i: (3, 0, 0)),
            VM,
            VM,
        ],
        out_specs=[VM, VM, VM],
        name="center",
        compiler_params=pltpu.CompilerParams(vmem_limit_bytes=LIMIT),
        cost_estimate=pl.CostEstimate(flops=20_000_000, bytes_accessed=1000, transcendentals=0),
    )(source, iterate, last, conduct)


def edges_body(above, below, low_c, high_c, low, high):
    place, ends = lax.axis_index("sx"), lax.axis_size("sx") - 1
    low[HALO : HALO + N, :] = low_c[...]
    high[HALO : HALO + N, :] = high_c[...]
    for ref, base, present in ((above, 0, flag(place > 0)), (below, HALO + N, flag(place < ends))):
        pieces = [(ref[f, :, :128] * present, ref[f, :, 128:] * present) for f in range(FIELDS)]
        lo, hi = pack_edges(pieces, HALO)
        for k in range(2):
            low[base : base + HALO, 128 * k : 128 * k + 128] = lo[k]
            high[base : base + HALO, 128 * k : 128 * k + 128] = hi[k]


def side_column(before, after, f, rows, first, final):
    lane = lanes(rows)
    at = HALO * (f % 8)
    right = jnp.where(lane < HALO, roll(after, -at) * final, 0.0)
    return jnp.where(lane >= 128 - HALO, roll(before, -HALO - at) * first, right)


MAIN_ROWS = 272
PART1 = 2 * MAIN_ROWS
PART2 = PART1 + 4 * HALO
MAIN = PART2 + EXT // 2


def window(x, width):
    return roll(x, width)


def fold(dest, base, columns, width, groups, rows_in):
    span = 2 * width
    rows = rows_in // groups
    lane = lanes(rows)
    out = jnp.zeros((rows, 128), F32)
    for g in range(groups):
        for k, read in enumerate(columns):
            at = (g * len(columns) + k) * span
            inside = (lane >= at) & (lane < at + span)
            out = jnp.where(inside, roll(read(g * rows, rows), width + at), out)
    dest[base : base + rows, :] = out


def unfold(src, base, k, count, width, groups, rows_in, write):
    span = 2 * width
    rows = rows_in // groups
    lane = lanes(rows)
    for g in range(groups):
        at = (g * count + k) * span
        x = roll(src[base : base + rows, :], -width - at)
        write(g * rows, rows, jnp.where((lane < width) | (lane >= 128 - width), x, 0.0))


def local_body(
    ext_in, above, below, before, after,
    ext, coefs, forced, own_new, main, up, down, low_c, high_c, coarse,
    rhs, mid, scaled,
):
    del ext_in
    t, x, z = lax.axis_index("tm"), lax.axis_index("sx"), lax.axis_index("sy")
    not_end = flag(t < lax.axis_size("tm") - 1)
    x_first, x_final = flag(x > 0), flag(x < lax.axis_size("sx") - 1)
    z_first, z_final = flag(z > 0), flag(z < lax.axis_size("sy") - 1)
    inv, cof = coefs.at[0], coefs.at[1]
    for f in range(FIELDS):
        for j in range(2):
            ext[f, j, PAD:TOP, :] = above[f, :, 128 * j : 128 * j + 128] * x_first
            ext[f, j, TOP + N : TOP + N + HALO, :] = below[f, :, 128 * j : 128 * j + 128] * x_final

    def columns(base):
        at = pl.ds(base - PAD, 32)
        for k in range(2):
            left, right = before[at, 128 * k : 128 * k + 128], after[at, 128 * k : 128 * k + 128]
            for f in range(8 * k, min(8 * k + 8, FIELDS)):
                ext[f, 2, pl.ds(base, 32), :] = side_column(left, right, f, 32, z_first, z_final)

    loop(EXT, 32, columns)
    clear_pads((rhs, mid), 3, 3, EXT)

    def prepare(base):
        at = pl.ds(base, 32)
        for j in range(3):
            c = ext[COEF, j, at, :]
            r = 1.0 / (1.0 + 4.0 * c)
            inv[j, at, :] = r
            cof[j, at, :] = c * r
            rhs[0, j, at, :] = ext[MID, j, at, :] + ext[4, j, at, :]
            rhs[1, j, at, :] = ext[0, j, at, :]
            rhs[2, j, at, :] = ext[LAST, j, at, :]

    loop(EXT, 32, prepare)
    for k in range(1, FACTOR):

        def add(f, j, at, u, k=k):
            return u + ext[4 + k, j, at, :] if f == 0 else u + ext[k, j, at, :] if f == 1 else u

        step(rhs, mid, scaled, inv, cof, range(3), 3, EXT, 32, add)
    step(rhs, mid, scaled, inv, cof, range(3), 3, EXT, 32, keep)

    def between(base):
        at = pl.ds(base, 32)
        for j in range(3):
            new, old = rhs[0, j, at, :], ext[LAST, j, at, :]
            scaled[0, j, at, :] = old + not_end * (new - old)
            if j < 2:
                own_new[j, at, :] = new
            rhs[0, j, at, :] = not_end * (new - old)
            s = rhs[1, j, at, :]
            forced[j, at, :] = s
            rhs[1, j, at, :] = s - ext[MID, j, at, :]

    loop(EXT, 32, between)
    for j in range(2):
        main[MAIN_ROWS * j : MAIN_ROWS * (j + 1), :] = scaled[0, j, 2 * PAD : 2 * PAD + MAIN_ROWS, :]
        main[PART1 + 2 * HALO * j : PART1 + 2 * HALO * j + HALO, :] = ext[LAST, j, PAD:TOP, :]
        main[PART1 + 2 * HALO * j + HALO : PART1 + 2 * HALO * (j + 1), :] = ext[LAST, j, TOP + N : TOP + N + HALO, :]
    fold(
        main, PART2,
        [lambda r, n: scaled[0, 2, PAD + r : PAD + r + n, :], lambda r, n: ext[LAST, 2, PAD + r : PAD + r + n, :]],
        HALO, 2, EXT,
    )
    for k in range(FACTOR):
        step(rhs, mid, scaled, inv, cof, range(3), 3, EXT, 32, keep)
    coarse[0] = restrict(rhs, 1, TOP)
    coarse[1] = restrict(rhs, 0, TOP)
    coarse[2] = restrict(rhs, 2, TOP)
    coarse[3] = restrict(ext, COEF, TOP)
    for k in range(4):
        up[k] = coarse[k, 0:HALO, :]
        down[k] = coarse[k, C - HALO : C, :]
    lo, hi = pack_edges([(coarse[k], coarse[k]) for k in range(4)], C)
    low_c[...] = lo[0]
    high_c[...] = hi[0]


def coarse_edges_body(above, below, low_c, high_c, low, high):
    place, ends = lax.axis_index("sx"), lax.axis_size("sx") - 1
    low[HALO : HALO + C, :] = low_c[...]
    high[HALO : HALO + C, :] = high_c[...]
    for ref, base, present in ((above, 0, flag(place > 0)), (below, HALO + C, flag(place < ends))):
        lo, hi = pack_edges([(ref[k] * present,) * 2 for k in range(4)], HALO)
        low[base : base + HALO, :] = lo[0]
        high[base : base + HALO, :] = hi[0]


SENT = 144
SENT_AT = 2 * PAD


def coarse_body(coarse, above, below, before, after, one, two, three, four, coefs, ext, rhs, mid, scaled):
    t, x, z = lax.axis_index("tm"), lax.axis_index("sx"), lax.axis_index("sy")
    not_end = flag(t < lax.axis_size("tm") - 1)
    x_first, x_final = flag(x > 0), flag(x < lax.axis_size("sx") - 1)
    z_first, z_final = flag(z > 0), flag(z < lax.axis_size("sy") - 1)
    for k in range(4):
        ext[k, 0, PAD:TOP, :] = above[k] * x_first
        ext[k, 0, TOP : TOP + C, :] = coarse[k]
        ext[k, 0, TOP + C : TOP + C + HALO, :] = below[k] * x_final
        ext[k, 1, PAD : PAD + CEXT, :] = side_column(before[...], after[...], k, CEXT, z_first, z_final)
    inv, cof = coefs.at[0], coefs.at[1]
    clear_pads((rhs, mid), 2, 2, CEXT)
    own = pl.ds(PAD, CEXT)
    for j in range(2):
        c = ext[3, j, own, :]
        r = 1.0 / (1.0 + 4.0 * c)
        inv[j, own, :] = r
        cof[j, own, :] = c * r
        rhs[0, j, own, :] = ext[0, j, own, :] * not_end
        rhs[1, j, own, :] = ext[1, j, own, :]

    def advance(fields, after_step):
        step(rhs, mid, scaled, inv, cof, fields, 2, CEXT, 32, after_step)

    advance(range(2), lambda f, j, at, u: u if f == 0 else u + ext[2, j, at, :])
    for j in range(2):
        ext[2, j, own, :] = rhs[1, j, own, :]
    advance(range(2), lambda f, j, at, u: u + ext[2, j, at, :] if f == 0 else u)
    rows = slice(SENT_AT, SENT_AT + SENT)

    def reader(ref, f):
        return lambda r, n: ref[f, 1, SENT_AT + r : SENT_AT + r + n, :]

    one[0:SENT, :] = ext[0, 0, rows, :]
    one[SENT : 2 * SENT, :] = ext[1, 0, rows, :]
    fold(one, 2 * SENT, [reader(ext, 0), reader(ext, 1)], 8, 3, SENT)
    two[0:SENT, :] = rhs[0, 0, rows, :]
    fold(two, SENT, [reader(rhs, 0)], 8, 6, SENT)
    advance(range(2), keep)
    advance(range(2), keep)
    three[0:SENT, :] = rhs[0, 0, rows, :]
    fold(three, SENT, [reader(rhs, 0)], 8, 6, SENT)
    advance(range(1, 2), keep)
    for j in range(2):
        four[j] = rhs[1, j, rows, :]


def arrive_body(last, main, ext, coefs, forced, resid, new_start, new_mid, coarse_mid, rhs, mid, scaled):
    inv, cof = coefs.at[0], coefs.at[1]
    clear_pads((rhs, mid), 2, 3, EXT)
    for j in range(2):
        rhs[0, j, PAD:TOP, :] = main[PART1 + 2 * HALO * j : PART1 + 2 * HALO * j + HALO, :]
        rhs[0, j, TOP : TOP + N, :] = last[:, 128 * j : 128 * j + 128]
        rhs[0, j, TOP + N : TOP + N + HALO, :] = main[PART1 + 2 * HALO * j + HALO : PART1 + 2 * HALO * (j + 1), :]
        new_start[j, PAD : 2 * PAD, :] = jnp.zeros((PAD, 128), F32)
        new_start[j, 2 * PAD : 2 * PAD + MAIN_ROWS, :] = main[MAIN_ROWS * j : MAIN_ROWS * (j + 1), :]
        new_start[j, 2 * PAD + MAIN_ROWS : 3 * PAD + MAIN_ROWS, :] = jnp.zeros((PAD, 128), F32)

    def put_new(r, n, value):
        new_start[2, PAD + r : PAD + r + n, :] = value

    def put_old(r, n, value):
        rhs[0, 2, PAD + r : PAD + r + n, :] = value

    unfold(main, PART2, 0, 2, HALO, 2, EXT, put_new)
    unfold(main, PART2, 1, 2, HALO, 2, EXT, put_old)

    def difference(base):
        at = pl.ds(base, 32)
        for j in range(3):
            rhs[1, j, at, :] = new_start[j, at, :] - rhs[0, j, at, :]

    loop(EXT, 32, difference)
    for k in range(FACTOR):
        step(rhs, mid, scaled, inv, cof, range(2), 3, EXT, 32, keep)

    def between(base):
        at = pl.ds(base, 32)
        for j in range(3):
            u = rhs[0, j, at, :] + forced[j, at, :]
            new_mid[j, at, :] = u
            rhs[0, j, at, :] = u - ext[MID, j, at, :]

    loop(EXT, 32, between)
    for k in range(FACTOR):
        step(rhs, mid, scaled, inv, cof, range(1), 3, EXT, 32, keep)
    for k in range(2):
        for j in range(2):
            resid[k, :, 128 * j : 128 * j + 128] = rhs[1 - k, j, TOP : TOP + N, :]
    coarse_mid[...] = restrict(rhs, 0, TOP)


def final_body(
    one, two, three, four, ccoefs, coarse_mid, ext, coefs, new_start, new_mid, own_new,
    out, err, cmid, cscaled, fix, rhs, mid, scaled,
):
    t = lax.axis_index("tm")
    m1, m2, m3, m4 = flag(t > 0), flag(t > 0), flag(t > 1), flag(t > 2)
    inv, cof = ccoefs.at[0], ccoefs.at[1]
    clear_pads((err, cmid), 1, 2, CEXT)
    rows = slice(SENT_AT, SENT_AT + SENT)
    zero = jnp.zeros((PAD, 128), F32)
    for j in range(2):
        err[0, j, PAD:SENT_AT, :] = zero
        err[0, j, SENT_AT + SENT : SENT_AT + SENT + PAD, :] = zero
        cmid[0, j, PAD:SENT_AT, :] = zero
        cmid[0, j, SENT_AT + SENT : SENT_AT + SENT + PAD, :] = zero
    holds = (scaled.at[0, 1], scaled.at[0, 2], scaled.at[1, 1], scaled.at[1, 2])

    def put(ref):
        def write(r, n, value):
            ref[r : r + n, :] = value

        return write

    unfold(one, 2 * SENT, 0, 2, 8, 3, SENT, put(holds[0]))
    unfold(one, 2 * SENT, 1, 2, 8, 3, SENT, put(holds[1]))
    unfold(two, SENT, 0, 1, 8, 6, SENT, put(holds[2]))
    unfold(three, SENT, 0, 1, 8, 6, SENT, put(holds[3]))
    err[0, 0, rows, :] = m1 * one[0:SENT, :] + m2 * two[0:SENT, :] + m3 * three[0:SENT, :] + m4 * four[0]
    err[0, 1, rows, :] = (
        m1 * holds[0][0:SENT, :] + m2 * holds[2][0:SENT, :] + m3 * holds[3][0:SENT, :] + m4 * four[1]
    )

    def spread(k, sides):
        count = C + 8 if sides else C
        base = TOP - 4 if sides else TOP
        to = TOP - 8 if sides else TOP
        src = lax.broadcasted_iota(jnp.int32, (128, 128), 0)
        dst = lax.broadcasted_iota(jnp.int32, (128, 128), 1)
        for j in range(3 if sides else 2):
            if j < 2:
                pick = src == dst // 2 + 64 * j
            else:
                pick = ((dst < HALO) & (src == dst // 2)) | ((dst >= 128 - HALO) & (src == 64 + dst // 2))
            wide = jnp.dot(
                err[0, j // 2, base : base + count, :], flag(pick), precision=lax.Precision.HIGHEST,
                preferred_element_type=F32,
            )
            fix[k, j, pl.ds(to, count, stride=2), :] = wide
            fix[k, j, pl.ds(to + 1, count, stride=2), :] = wide

    clear_pads((rhs, mid), 2, 3, EXT)
    for k in range(2):
        for j in range(3):
            fix[k, j, PAD : TOP - 8, :] = zero
            fix[k, j, TOP + N + 8 : TOP + N + HALO, :] = zero
    spread(0, True)
    step(err, cmid, cscaled, inv, cof, range(1), 2, CEXT, 32, keep)
    err[0, 0, rows, :] += one[SENT : 2 * SENT, :]
    err[0, 1, rows, :] += holds[1][0:SENT, :]
    spread(1, True)
    step(err, cmid, cscaled, inv, cof, range(1), 2, CEXT, 32, keep)
    err[0, 0, TOP : TOP + C, :] += coarse_mid[...]
    spread(2, False)
    inv, cof = coefs.at[0], coefs.at[1]

    def begin(base):
        at = pl.ds(base, 32)
        for j in range(3):
            rhs[0, j, at, :] = new_start[j, at, :] + fix[0, j, at, :] + ext[0, j, at, :]
            u = new_mid[j, at, :] + fix[1, j, at, :]
            new_mid[j, at, :] = u
            rhs[1, j, at, :] = u + ext[4, j, at, :]

    loop(EXT, 32, begin)
    for j in range(2):
        cols = slice(128 * j, 128 * j + 128)
        out[3, :, cols] = new_mid[j, TOP : TOP + N, :]
        out[7, :, cols] = own_new[j, TOP : TOP + N, :] + fix[2, j, TOP : TOP + N, :]
    for k in range(FACTOR - 1):
        step(rhs, mid, scaled, inv, cof, range(2), 3, EXT, 32, keep)
        for f in range(2):
            for j in range(2):
                out[4 * f + k, :, 128 * j : 128 * j + 128] = rhs[f, j, TOP : TOP + N, :]
        if k + 1 < FACTOR - 1:

            def force(base, k=k):
                at = pl.ds(base, 32)
                for f in range(2):
                    for j in range(3):
                        rhs[f, j, at, :] += ext[4 * f + k + 1, j, at, :]

            loop(EXT, 32, force)


def ring(x, axis, by):
    count = lax.axis_size(axis)
    return lax.ppermute(x, axis, [(i, (i + by) % count) for i in range(count)])


def fine_scratch(fields):
    return [pltpu.VMEM((fields, 3, ROWS, 128), F32)] * 3


def shards(iterate, source, start_field, conduct):
    up, down, last = make_strips(iterate, source, start_field, conduct)
    above, below = ring(down, "sx", 1), ring(up, "sx", -1)
    last_in = ring(last, "tm", 1)
    ext, low_c, high_c = make_center(source, iterate, last, conduct)
    low, high = call(edges_body, [(EXT, 256)] * 2, 4, name="edges", flops=1_000_000)(above, below, low_c, high_c)
    before, after = ring(high, "sy", 1), ring(low, "sy", -1)
    ext, coefs, forced, own_new, main, c_up, c_down, c_low, c_high, coarse = call(
        local_body,
        [
            (FIELDS, 3, ROWS, 128), (2, 3, ROWS, 128), (3, ROWS, 128), (2, ROWS, 128), (MAIN, 128),
            (4, HALO, 128), (4, HALO, 128), (C, 128), (C, 128), (4, C, 128),
        ],
        5, fine_scratch(3), {0: 0}, "local", 50_000_000,
    )(ext, above, below, before, after)
    c_above, c_below = ring(c_down, "sx", 1), ring(c_up, "sx", -1)
    main_in = ring(main, "tm", 1)
    c_lo, c_hi = call(coarse_edges_body, [(CEXT, 128)] * 2, 4, name="coarse_edges")(c_above, c_below, c_low, c_high)
    c_before, c_after = ring(c_hi, "sy", 1), ring(c_lo, "sy", -1)
    one, two, three, four, ccoefs = call(
        coarse_body,
        [(2 * SENT + 48, 128), (SENT + 24, 128), (SENT + 24, 128), (2, SENT, 128), (2, 2, CROWS, 128)],
        5,
        [pltpu.VMEM((4, 2, CROWS, 128), F32)] + [pltpu.VMEM((2, 2, CROWS, 128), F32)] * 3,
        name="coarse",
    )(coarse, c_above, c_below, c_before, c_after)
    one, two, three = ring(one, "tm", 1), ring(two, "tm", 2), ring(three, "tm", 3)
    resid, new_start, new_mid, coarse_mid = call(
        arrive_body,
        [(2, N, N), (3, ROWS, 128), (3, ROWS, 128), (C, C)],
        5, fine_scratch(2), name="arrive", flops=30_000_000,
    )(last_in, main_in, ext, coefs, forced)
    (updated,) = call(
        final_body,
        [(8, N, N)],
        11,
        [pltpu.VMEM((1, 2, CROWS, 128), F32)] * 3 + [pltpu.VMEM((3, 3, ROWS, 128), F32)] + fine_scratch(2),
        name="final",
    )(one, two, three, four, ccoefs, coarse_mid, ext, coefs, new_start, new_mid, own_new)
    return updated, resid


def solution(mesh):
    in_specs = (P("tm", "sx", "sy"), P("tm", "sx", "sy"), P("sx", "sy"), P("sx", "sy"))
    out_specs = (P("tm", "sx", "sy"), P("tm", "sx", "sy"))
    return jax.shard_map(shards, mesh=mesh, in_specs=in_specs, out_specs=out_specs, check_vma=False)
```

```python
import jax
import jax.numpy as jnp
from jax import lax
from jax.experimental import pallas as pl
from jax.experimental.pallas import tpu as pltpu
from jax.sharding import PartitionSpec as P

FACTOR = 4
N = 256
HALO = 16
EXT = N + 2 * HALO
V = EXT // 8
C = N // 2
CEXT = C + 2 * HALO
CV = CEXT // 8
HALF = EXT // 2
HV = HALF // 8
FIELDS = 11
MID, LAST, COEF = 8, 9, 10
F32 = jnp.float32
LIMIT = 24 * 1024 * 1024

VM = pl.BlockSpec(memory_space=pltpu.VMEM)
HB = pl.BlockSpec(memory_space=pltpu.HBM)


def call(body, outs, ins, scratch=(), aliases=None, name=None, flops=0):
    return pl.pallas_call(
        body,
        out_shape=[jax.ShapeDtypeStruct(s, F32) for s in outs],
        in_specs=[VM] * ins if isinstance(ins, int) else ins,
        out_specs=[VM] * len(outs),
        scratch_shapes=list(scratch),
        input_output_aliases=aliases or {},
        name=name,
        compiler_params=pltpu.CompilerParams(vmem_limit_bytes=LIMIT),
        cost_estimate=pl.CostEstimate(flops=flops, bytes_accessed=1000, transcendentals=0),
    )


def lanes(rows):
    return lax.broadcasted_iota(jnp.int32, (rows, 128), 1)


def roll(x, by):
    by %= 128
    return pltpu.roll(x, by, 1) if by else x


def flag(condition):
    return jnp.where(condition, 1.0, 0.0).astype(F32)


def vec(v):
    return slice(8 * v, 8 * v + 8)


def mix(dest, read, count):
    for v in range(count):
        dest[vec(v), :] = read(v)


def natural(ref, count, offset=0):
    return lambda v: ref[pl.ds(offset + v, 8, stride=count), :]


def unmix(dest, read, count):
    for v in range(count):
        dest[pl.ds(v, 8, stride=count), :] = read(v)


def sweep(src, fields, cols, count, emit):
    lane = lanes(8)
    first, last = lane == 0, lane == 127
    held = {}

    def at(f, j, v):
        if (f, j, v) not in held:
            held[f, j, v] = src[f, j, vec(v), :]
        return held[f, j, v]

    for v in range(count):
        for f in fields:
            mid = [at(f, j, v) for j in range(cols)]
            left = [pltpu.roll(m, 1, 1) for m in mid]
            right = [pltpu.roll(m, 127, 1) for m in mid]
            for j in range(cols):
                below = at(f, j, v + 1) if v + 1 < count else pltpu.roll(src[f, j, vec(0), :], 7, 0)
                above = at(f, j, v - 1) if v else pltpu.roll(src[f, j, vec(count - 1), :], 1, 0)
                side = jnp.where(first, left[j - 1], left[j]) + jnp.where(last, right[(j + 1) % cols], right[j])
                emit(f, j, v, mid[j], (below + above) + side)
        for key in [k for k in held if k[2] < v]:
            del held[key]


def step(rhs, mid, scaled, inv, cof, fields, cols, count, after):
    def one(f, j, v, own, total):
        b = own * inv[j, vec(v), :]
        scaled[f, j, vec(v), :] = b
        mid[f, j, vec(v), :] = b + cof[j, vec(v), :] * total

    def two(f, j, v, own, total):
        u = scaled[f, j, vec(v), :] + cof[j, vec(v), :] * total
        rhs[f, j, vec(v), :] = after(f, j, v, u)

    sweep(rhs, fields, cols, count, one)
    sweep(mid, fields, cols, count, two)


def keep(f, j, v, u):
    return u


def repeat(count, body):
    def one(k, carry):
        body(k)
        return carry

    lax.fori_loop(0, count, one, 0)


def restrict(ref, f, pair):
    fine = lax.broadcasted_iota(jnp.int32, (128, C), 0) // 2
    coarse = lax.broadcasted_iota(jnp.int32, (128, C), 1)
    out = None
    for j in range(2):
        for i in range(HV):
            pair[vec(i), :] = ref[f, j, vec(2 * i), :] + ref[f, j, vec(2 * i + 1), :]
        pick = jnp.where(fine + 64 * j == coarse, 0.25, 0.0).astype(F32)
        part = jnp.dot(pair[...], pick, precision=lax.Precision.HIGHEST, preferred_element_type=F32)
        out = part if out is None else out + part
    return out


def strips_body(source, iterate, start, conduct, up, down, last, sems):
    is_end = lax.axis_index("tm") == lax.axis_size("tm") - 1
    low, high = pl.ds(0, HALO), pl.ds(N - HALO, HALO)
    copies = []
    for ref, rows in ((up, low), (down, high)):
        copies.append((source.at[:, rows, :], ref.at[pl.ds(0, 8)]))
        copies.append((iterate.at[3, rows, :], ref.at[MID]))
        copies.append((conduct.at[rows, :], ref.at[COEF]))
    copies = [pltpu.make_async_copy(a, b, sems.at[i]) for i, (a, b) in enumerate(copies)]
    for c in copies:
        c.start()

    @pl.when(is_end)
    def _():
        c = pltpu.make_async_copy(start, last, sems.at[6])
        c.start()
        c.wait()

    @pl.when(jnp.logical_not(is_end))
    def _():
        c = pltpu.make_async_copy(iterate.at[7], last, sems.at[6])
        c.start()
        c.wait()

    up[LAST] = last[0:HALO, :]
    down[LAST] = last[N - HALO : N, :]
    for c in copies:
        c.wait()


def pack_edges(pieces, rows):
    lane = lanes(rows)
    low = [jnp.zeros((rows, 128), F32) for _ in range((len(pieces) + 7) // 8)]
    high = list(low)
    for f, (head, tail) in enumerate(pieces):
        at, k = HALO * (f % 8), f // 8
        inside = (lane >= at) & (lane < at + HALO)
        low[k] = jnp.where(inside, roll(head, at), low[k])
        high[k] = jnp.where(inside, roll(tail, at + HALO), high[k])
    return low, high


REST = HALO * (FIELDS - 8)


def center_body(source, iterate, last, conduct, ext, low, high, src, middle, coef, wide, sems):
    pairs = ((source, src), (iterate.at[3], middle), (conduct, coef))
    copies = [pltpu.make_async_copy(a, b, sems.at[i]) for i, (a, b) in enumerate(pairs)]
    for c in copies:
        c.start()
    for c in copies:
        c.wait()
    refs = [src.at[f] for f in range(8)] + [middle, last, coef]
    rows = 16

    def chunk(i, carry):
        base = pl.multiple_of(i * rows, 8)
        pieces = [(ref[pl.ds(base, rows), :128], ref[pl.ds(base, rows), 128:]) for ref in refs]
        lo, hi = pack_edges(pieces, rows)
        for ref, got in ((low, lo), (high, hi)):
            ref[pl.ds(base, rows), :] = got[0]
            @pl.when(i < 8)
            def _(ref=ref, got=got):
                ref[pl.ds(N + base, rows), :] = got[1]

            @pl.when(i >= 8)
            def _(ref=ref, got=got):
                at = pl.ds(N + base - 128, rows)
                ref[at, :] = jnp.where(lanes(rows) < REST, ref[at, :], roll(got[1], REST))
        return carry

    lax.fori_loop(0, N // rows, chunk, 0)
    zero = jnp.zeros((HALO, 128), F32)
    wide[0:HALO, :] = zero
    wide[HALO + N : EXT, :] = zero
    for f, ref in enumerate(refs):
        for j in range(2):
            wide[HALO : HALO + N, :] = ref[:, 128 * j : 128 * j + 128]
            mix(ext.at[f, j], natural(wide, V), V)


def corners_body(above, below, low, high):
    place, ends = lax.axis_index("sx"), lax.axis_size("sx") - 1
    lane = lanes(HALO)
    got = []
    for ref, present in ((above, flag(place > 0)), (below, flag(place < ends))):
        pieces = [(ref[f, :, :128] * present, ref[f, :, 128:] * present) for f in range(FIELDS)]
        got.append(pack_edges(pieces, HALO))
    for k, ref in ((0, low), (1, high)):
        ref[0:HALO, :] = got[0][k][0]
        ref[HALO : 2 * HALO, :] = got[1][k][0]
        ref[2 * HALO : 3 * HALO, :] = jnp.where(lane < REST, got[0][k][1], roll(got[1][k][1], REST))


def side_column(before, after, f, rows, first, final):
    lane = lanes(rows)
    at = HALO * (f % 8)
    right = jnp.where(lane < HALO, roll(after, -at) * final, 0.0)
    return jnp.where(lane >= 128 - HALO, roll(before, -HALO - at) * first, right)


PART1 = 2 * EXT
PART2 = PART1 + 4 * HALO
MAIN = PART2 + EXT // 2


def fold(dest, base, columns, width, groups, rows_in):
    span = 2 * width
    rows = rows_in // groups
    lane = lanes(rows)
    out = jnp.zeros((rows, 128), F32)
    for g in range(groups):
        for k, read in enumerate(columns):
            at = (g * len(columns) + k) * span
            inside = (lane >= at) & (lane < at + span)
            out = jnp.where(inside, roll(read(g * rows, rows), width + at), out)
    dest[base : base + rows, :] = out


def unfold(src, base, k, count, width, groups, rows_in, write):
    span = 2 * width
    rows = rows_in // groups
    lane = lanes(rows)
    for g in range(groups):
        at = (g * count + k) * span
        x = roll(src[base : base + rows, :], -width - at)
        write(g * rows, rows, jnp.where((lane < width) | (lane >= 128 - width), x, 0.0))


def local_body(
    ext_in, above, below, before, after, before_c, after_c,
    ext, coefs, forced, own_new, main, up, down, low_c, high_c, coarse,
    rhs, mid, scaled, wide, pair, rows_c,
):
    del ext_in
    t, x, z = lax.axis_index("tm"), lax.axis_index("sx"), lax.axis_index("sy")
    not_end = flag(t < lax.axis_size("tm") - 1)
    x_first, x_final = flag(x > 0), flag(x < lax.axis_size("sx") - 1)
    z_first, z_final = flag(z > 0), flag(z < lax.axis_size("sy") - 1)
    inv, cof = coefs.at[0], coefs.at[1]
    for f in range(FIELDS):
        for j in range(2):
            cols = slice(128 * j, 128 * j + 128)
            for h in range(2):
                part = slice(8 * h, 8 * h + 8)
                ext[f, j, pl.ds(64 * h, 8, stride=8), :] = above[f, part, cols] * x_first
                ext[f, j, pl.ds(8 * (V - HALO) + 64 * h + 7, 8, stride=8), :] = below[f, part, cols] * x_final
    for k, (own, corner) in enumerate(((before, before_c), (after, after_c))):
        wide[k, 0, 0:HALO, :] = corner[0:HALO, :]
        wide[k, 0, HALO : HALO + N, :] = own[0:N, :]
        wide[k, 0, HALO + N : EXT, :] = corner[HALO : 2 * HALO, :]
        rest = corner[2 * HALO : 3 * HALO, :]
        wide[k, 1, 0:HALO, :] = rest
        wide[k, 1, HALO : HALO + 128, :] = own[N : N + 128, :]
        wide[k, 1, HALO + 128 : HALO + N, :] = roll(own[N : N + 128, :], -REST)
        wide[k, 1, HALO + N : EXT, :] = roll(rest, -REST)
    for v in range(V):
        for g in range(2):
            left, right = natural(wide.at[0, g], V)(v), natural(wide.at[1, g], V)(v)
            for f in range(8 * g, min(8 * g + 8, FIELDS)):
                ext[f, 2, vec(v), :] = side_column(left, right, f, 8, z_first, z_final)
    for v in range(V):
        for j in range(3):
            c = ext[COEF, j, vec(v), :]
            r = 1.0 / (1.0 + 4.0 * c)
            inv[j, vec(v), :] = r
            cof[j, vec(v), :] = c * r
            rhs[0, j, vec(v), :] = ext[MID, j, vec(v), :] + ext[4, j, vec(v), :]
            rhs[1, j, vec(v), :] = ext[0, j, vec(v), :]
            rhs[2, j, vec(v), :] = ext[LAST, j, vec(v), :]

    def forced_step(k):
        def add(f, j, v, u):
            return u if f == 2 else u + ext[(5 if f == 0 else 1) + k, j, vec(v), :]

        step(rhs, mid, scaled, inv, cof, range(3), 3, V, add)

    repeat(FACTOR - 1, forced_step)

    def between():
        for v in range(V):
            for j in range(3):
                new, old = rhs[0, j, vec(v), :], ext[LAST, j, vec(v), :]
                moved = not_end * (new - old)
                if j < 2:
                    own_new[j, vec(v), :] = new
                    main[EXT * j + 8 * v : EXT * j + 8 * v + 8, :] = old + moved
                else:
                    scaled[0, j, vec(v), :] = old + moved
                rhs[0, j, vec(v), :] = moved
                s = rhs[1, j, vec(v), :]
                forced[j, vec(v), :] = s
                rhs[1, j, vec(v), :] = s - ext[MID, j, vec(v), :]
        for j in range(2):
            cols = slice(128 * j, 128 * j + 128)
            at = PART1 + 2 * HALO * j
            main[at : at + HALO, :] = above[LAST, :, cols] * x_first
            main[at + HALO : at + 2 * HALO, :] = below[LAST, :, cols] * x_final
        fold(
            main, PART2,
            [lambda r, n: scaled[0, 2, r : r + n, :], lambda r, n: ext[LAST, 2, r : r + n, :]],
            HALO, 2, EXT,
        )

    def free_step(k):
        step(rhs, mid, scaled, inv, cof, range(3), 3, V, keep)
        pl.when(k == 0)(between)

    repeat(FACTOR + 1, free_step)
    for k, (ref, f) in enumerate(((rhs, 1), (rhs, 0), (rhs, 2), (ext, COEF))):
        got = restrict(ref, f, pair)
        pair[...] = got
        unmix(rows_c, lambda v: pair[vec(v), :], HV)
        coarse[k] = rows_c[8 : 8 + C, :]
    for k in range(4):
        up[k] = coarse[k, 0:HALO, :]
        down[k] = coarse[k, C - HALO : C, :]
    lo, hi = pack_edges([(coarse[k], coarse[k]) for k in range(4)], C)
    low_c[...] = lo[0]
    high_c[...] = hi[0]


def coarse_edges_body(above, below, low_c, high_c, low, high):
    place, ends = lax.axis_index("sx"), lax.axis_size("sx") - 1
    low[HALO : HALO + C, :] = low_c[...]
    high[HALO : HALO + C, :] = high_c[...]
    for ref, base, present in ((above, 0, flag(place > 0)), (below, HALO + C, flag(place < ends))):
        lo, hi = pack_edges([(ref[k] * present,) * 2 for k in range(4)], HALO)
        low[base : base + HALO, :] = lo[0]
        high[base : base + HALO, :] = hi[0]


ONE = 2 * CEXT + CEXT // 4
TWO = CEXT + CEXT // 5


def coarse_body(coarse, above, below, before, after, one, two, three, four, coefs, ext, rhs, mid, scaled, wide):
    t, x, z = lax.axis_index("tm"), lax.axis_index("sx"), lax.axis_index("sy")
    not_end = flag(t < lax.axis_size("tm") - 1)
    x_first, x_final = flag(x > 0), flag(x < lax.axis_size("sx") - 1)
    z_first, z_final = flag(z > 0), flag(z < lax.axis_size("sy") - 1)
    for k in range(4):
        wide[0:HALO, :] = above[k] * x_first
        wide[HALO : HALO + C, :] = coarse[k]
        wide[HALO + C : CEXT, :] = below[k] * x_final
        mix(ext.at[k, 0], natural(wide, CV), CV)
    for v in range(CV):
        left, right = natural(before, CV)(v), natural(after, CV)(v)
        for k in range(4):
            ext[k, 1, vec(v), :] = side_column(left, right, k, 8, z_first, z_final)
    inv, cof = coefs.at[0], coefs.at[1]
    for j in range(2):
        c = ext[3, j]
        r = 1.0 / (1.0 + 4.0 * c)
        inv[j] = r
        cof[j] = c * r
        rhs[0, j] = ext[0, j] * not_end
        rhs[1, j] = ext[1, j]

    def advance(fields, after_step):
        step(rhs, mid, scaled, inv, cof, fields, 2, CV, after_step)

    def reader(ref, f):
        return lambda r, n: ref[f, 1, r : r + n, :]

    one[0:CEXT, :] = ext[0, 0]
    one[CEXT : 2 * CEXT, :] = ext[1, 0]
    fold(one, 2 * CEXT, [reader(ext, 0), reader(ext, 1)], 8, 4, CEXT)
    advance(range(2), lambda f, j, v, u: u if f == 0 else u + ext[2, j, vec(v), :])
    for j in range(2):
        ext[2, j] = rhs[1, j]
    advance(range(2), lambda f, j, v, u: u + ext[2, j, vec(v), :] if f == 0 else u)
    two[0:CEXT, :] = rhs[0, 0]
    fold(two, CEXT, [reader(rhs, 0)], 8, 5, CEXT)
    repeat(2, lambda k: advance(range(2), keep))
    three[0:CEXT, :] = rhs[0, 0]
    fold(three, CEXT, [reader(rhs, 0)], 8, 5, CEXT)
    advance(range(1, 2), keep)
    for j in range(2):
        four[j] = rhs[1, j]


def arrive_body(last, main, ext, coefs, forced, resid, new_start, new_mid, coarse_mid, rhs, mid, scaled, wide, pair):
    inv, cof = coefs.at[0], coefs.at[1]
    for j in range(2):
        at = PART1 + 2 * HALO * j
        wide[0:HALO, :] = main[at : at + HALO, :]
        wide[HALO : HALO + N, :] = last[:, 128 * j : 128 * j + 128]
        wide[HALO + N : EXT, :] = main[at + HALO : at + 2 * HALO, :]
        mix(rhs.at[0, j], natural(wide, V), V)
        new_start[j] = main[EXT * j : EXT * (j + 1), :]

    def put_new(r, n, value):
        new_start[2, r : r + n, :] = value

    def put_old(r, n, value):
        rhs[0, 2, r : r + n, :] = value

    unfold(main, PART2, 0, 2, HALO, 2, EXT, put_new)
    unfold(main, PART2, 1, 2, HALO, 2, EXT, put_old)
    for j in range(3):
        rhs[1, j] = new_start[j] - rhs[0, j]
    repeat(FACTOR, lambda k: step(rhs, mid, scaled, inv, cof, range(2), 3, V, keep))
    for j in range(3):
        for v in range(V):
            u = rhs[0, j, vec(v), :] + forced[j, vec(v), :]
            new_mid[j, vec(v), :] = u
            rhs[0, j, vec(v), :] = u - ext[MID, j, vec(v), :]
    repeat(FACTOR, lambda k: step(rhs, mid, scaled, inv, cof, range(1), 3, V, keep))
    for k in range(2):
        for j in range(2):
            unmix(wide, lambda v: rhs[1 - k, j, vec(v), :], V)
            resid[k, :, 128 * j : 128 * j + 128] = wide[HALO : HALO + N, :]
    coarse_mid[...] = restrict(rhs, 0, pair)


def final_body(
    one, two, three, four, ccoefs, coarse_mid, ext, coefs, new_start, new_mid, own_new,
    out, err, cmid, cscaled, sent, fix, rhs, mid, scaled, wide, pair, rows_c,
):
    t = lax.axis_index("tm")
    m1, m2, m3 = flag(t > 0), flag(t > 1), flag(t > 2)
    inv, cof = ccoefs.at[0], ccoefs.at[1]

    def put(k):
        def write(r, n, value):
            sent[k, r : r + n, :] = value

        return write

    unfold(one, 2 * CEXT, 0, 2, 8, 4, CEXT, put(0))
    unfold(one, 2 * CEXT, 1, 2, 8, 4, CEXT, put(1))
    unfold(two, CEXT, 0, 1, 8, 5, CEXT, put(2))
    unfold(three, CEXT, 0, 1, 8, 5, CEXT, put(3))
    err[0, 0] = m1 * (one[0:CEXT, :] + two[0:CEXT, :]) + m2 * three[0:CEXT, :] + m3 * four[0]
    err[0, 1] = m1 * (sent[0] + sent[2]) + m2 * sent[3] + m3 * four[1]

    def spread(k, extra=None):
        src = lax.broadcasted_iota(jnp.int32, (128, 128), 0)
        dst = lax.broadcasted_iota(jnp.int32, (128, 128), 1)
        for c in range(2 if extra is None else 1):
            unmix(rows_c, lambda v: err[0, c, vec(v), :], CV)
            mix(pair, natural(rows_c, HV, 8), HV)
            value = pair[...] if extra is None else pair[...] + extra[...]
            for j in (0, 1) if c == 0 else (2,):
                if c == 0:
                    pick = src == dst // 2 + 64 * j
                else:
                    pick = ((dst < HALO) & (src == dst // 2)) | ((dst >= 128 - HALO) & (src == 64 + dst // 2))
                fix[k, j] = jnp.dot(value, flag(pick), precision=lax.Precision.HIGHEST, preferred_element_type=F32)

    spread(0)
    step(err, cmid, cscaled, inv, cof, range(1), 2, CV, keep)
    err[0, 0] += one[CEXT : 2 * CEXT, :]
    err[0, 1] += sent[1]
    spread(1)
    step(err, cmid, cscaled, inv, cof, range(1), 2, CV, keep)
    spread(2, coarse_mid)
    inv, cof = coefs.at[0], coefs.at[1]
    for v in range(V):
        for j in range(3):
            rhs[0, j, vec(v), :] = new_start[j, vec(v), :] + fix[0, j, vec(v // 2), :] + ext[0, j, vec(v), :]
            u = new_mid[j, vec(v), :] + fix[1, j, vec(v // 2), :]
            scaled[0, j, vec(v), :] = u
            rhs[1, j, vec(v), :] = u + ext[4, j, vec(v), :]
            if j < 2:
                scaled[1, j, vec(v), :] = own_new[j, vec(v), :] + fix[2, j, vec(v // 2), :]

    def give(at):
        for f in range(2):
            for j in range(2):
                unmix(wide, lambda v: scaled[f, j, vec(v), :], V)
                out[4 * f + at, :, 128 * j : 128 * j + 128] = wide[HALO : HALO + N, :]

    give(FACTOR - 1)

    def fine(k):
        def add(f, j, v, u):
            scaled[f, j, vec(v), :] = u
            return u + ext[4 * f + 1 + k, j, vec(v), :]

        step(rhs, mid, scaled, inv, cof, range(2), 3, V, add)
        give(k)

    repeat(FACTOR - 1, fine)


def ring(x, axis, by):
    count = lax.axis_size(axis)
    return lax.ppermute(x, axis, [(i, (i + by) % count) for i in range(count)])


def vmem(*shape):
    return pltpu.VMEM(shape, F32)


def shards(iterate, source, start_field, conduct):
    up, down, last = call(
        strips_body, [(FIELDS, HALO, N)] * 2 + [(N, N)], [HB] * 4, [pltpu.SemaphoreType.DMA((7,))], name="strips"
    )(source, iterate, start_field, conduct)
    above, below = ring(down, "sx", 1), ring(up, "sx", -1)
    last_in = ring(last, "tm", 1)
    ext, low, high = call(
        center_body,
        [(FIELDS, 3, EXT, 128), (N + 128, 128), (N + 128, 128)],
        [HB, HB, VM, HB],
        [vmem(8, N, N), vmem(N, N), vmem(N, N), vmem(EXT, 128), pltpu.SemaphoreType.DMA((3,))],
        name="center", flops=20_000_000,
    )(source, iterate, last, conduct)
    before, after = ring(high, "sy", 1), ring(low, "sy", -1)
    c_lo, c_hi = call(corners_body, [(3 * HALO, 128)] * 2, 2, name="corners")(above, below)
    before_c, after_c = ring(c_hi, "sy", 1), ring(c_lo, "sy", -1)
    before, after, before_c, after_c, last_in = lax.optimization_barrier((before, after, before_c, after_c, last_in))
    ext, coefs, forced, own_new, main, c_up, c_down, c_low, c_high, coarse = call(
        local_body,
        [
            (FIELDS, 3, EXT, 128), (2, 3, EXT, 128), (3, EXT, 128), (2, EXT, 128), (MAIN, 128),
            (4, HALO, 128), (4, HALO, 128), (C, 128), (C, 128), (4, C, 128),
        ],
        7, [vmem(3, 3, EXT, 128)] * 3 + [vmem(2, 2, EXT, 128), vmem(HALF, 128), vmem(HALF, 128)],
        {0: 0}, "local", 50_000_000,
    )(ext, above, below, before, after, before_c, after_c)
    c_above, c_below = ring(c_down, "sx", 1), ring(c_up, "sx", -1)
    main_in = ring(main, "tm", 1)
    c_lo, c_hi = call(coarse_edges_body, [(CEXT, 128)] * 2, 4, name="coarse_edges")(c_above, c_below, c_low, c_high)
    c_before, c_after = ring(c_hi, "sy", 1), ring(c_lo, "sy", -1)
    one, two, three, four, ccoefs = call(
        coarse_body,
        [(ONE, 128), (TWO, 128), (TWO, 128), (2, CEXT, 128), (2, 2, CEXT, 128)],
        5,
        [vmem(4, 2, CEXT, 128)] + [vmem(2, 2, CEXT, 128)] * 3 + [vmem(CEXT, 128)],
        name="coarse",
    )(coarse, c_above, c_below, c_before, c_after)
    one, two, three = ring(one, "tm", 1), ring(two, "tm", 2), ring(three, "tm", 3)
    resid, new_start, new_mid, coarse_mid = call(
        arrive_body,
        [(2, N, N), (3, EXT, 128), (3, EXT, 128), (HALF, 128)],
        5, [vmem(2, 3, EXT, 128)] * 3 + [vmem(EXT, 128), vmem(HALF, 128)], name="arrive", flops=30_000_000,
    )(last_in, main_in, ext, coefs, forced)
    (updated,) = call(
        final_body,
        [(8, N, N)],
        11,
        [vmem(1, 2, CEXT, 128)] * 3 + [vmem(4, CEXT, 128), vmem(3, 3, HALF, 128)] + [vmem(2, 3, EXT, 128)] * 3
        + [vmem(EXT, 128), vmem(HALF, 128), vmem(CEXT, 128)],
        name="final",
    )(one, two, three, four, ccoefs, coarse_mid, ext, coefs, new_start, new_mid, own_new)
    return updated, resid


def solution(mesh):
    in_specs = (P("tm", "sx", "sy"), P("tm", "sx", "sy"), P("sx", "sy"), P("sx", "sy"))
    out_specs = (P("tm", "sx", "sy"), P("tm", "sx", "sy"))
    return jax.shard_map(shards, mesh=mesh, in_specs=in_specs, out_specs=out_specs, check_vma=False)
```

```python
import jax
import jax.numpy as jnp
from jax import lax
from jax.experimental import pallas as pl
from jax.experimental.pallas import tpu as pltpu
from jax.sharding import PartitionSpec as P

FACTOR = 4
N = 256
HALO = 16
EXT = N + 2 * HALO
V = EXT // 8
C = N // 2
CEXT = C + 2 * HALO
CV = CEXT // 8
HALF = EXT // 2
HV = HALF // 8
FIELDS = 11
MID, LAST, COEF = 8, 9, 10
LIVE = EXT // 3
F32 = jnp.float32
LIMIT = 24 * 1024 * 1024

VM = pl.BlockSpec(memory_space=pltpu.VMEM)
HB = pl.BlockSpec(memory_space=pltpu.HBM)


def call(body, outs, ins, scratch=(), aliases=None, name=None, flops=0, limit=LIMIT):
    return pl.pallas_call(
        body,
        out_shape=[jax.ShapeDtypeStruct(s, F32) for s in outs],
        in_specs=[VM] * ins if isinstance(ins, int) else ins,
        out_specs=[VM] * len(outs),
        scratch_shapes=list(scratch),
        input_output_aliases=aliases or {},
        name=name,
        compiler_params=pltpu.CompilerParams(vmem_limit_bytes=limit),
        cost_estimate=pl.CostEstimate(flops=flops, bytes_accessed=1000, transcendentals=0),
    )


def lanes(rows):
    return lax.broadcasted_iota(jnp.int32, (rows, 128), 1)


def roll(x, by):
    by %= 128
    return pltpu.roll(x, by, 1) if by else x


def flag(condition):
    return jnp.where(condition, 1.0, 0.0).astype(F32)


def vec(v):
    return slice(8 * v, 8 * v + 8)


def mix(dest, read, count):
    for v in range(count):
        dest[vec(v), :] = read(v)


def natural(ref, count, offset=0):
    return lambda v: ref[pl.ds(offset + v, 8, stride=count), :]


def unmix(dest, read, count):
    for v in range(count):
        dest[pl.ds(v, 8, stride=count), :] = read(v)


def sweep(src, fields, cols, count, emit):
    lane = lanes(8)
    first, last = lane == 0, lane == 127
    held = {}

    def at(f, j, v):
        if (f, j, v) not in held:
            held[f, j, v] = src[f, j, vec(v), :]
        return held[f, j, v]

    for v in range(count):
        for f in fields:
            mid = [at(f, j, v) for j in range(cols)]
            if cols == 3:
                left = [pltpu.roll(mid[2], 1, 1), mid[0], mid[1]]
                right = [mid[1], mid[2], pltpu.roll(mid[0], 127, 1)]
            else:
                back = [pltpu.roll(m, 1, 1) for m in mid]
                ahead = [pltpu.roll(m, 127, 1) for m in mid]
                left = [jnp.where(first, back[1 - j], back[j]) for j in range(2)]
                right = [jnp.where(last, ahead[1 - j], ahead[j]) for j in range(2)]
            for j in range(cols):
                below = at(f, j, v + 1) if v + 1 < count else pltpu.roll(src[f, j, vec(0), :], 7, 0)
                above = at(f, j, v - 1) if v else pltpu.roll(src[f, j, vec(count - 1), :], 1, 0)
                emit(f, j, v, mid[j], (below + above) + (left[j] + right[j]))
        for key in [k for k in held if k[2] < v]:
            del held[key]


def step(rhs, mid, scaled, inv, cof, fields, cols, count, after):
    def one(f, j, v, own, total):
        b = own * inv[j, vec(v), :]
        scaled[f, j, vec(v), :] = b
        mid[f, j, vec(v), :] = b + cof[j, vec(v), :] * total

    def two(f, j, v, own, total):
        u = scaled[f, j, vec(v), :] + cof[j, vec(v), :] * total
        rhs[f, j, vec(v), :] = after(f, j, v, u)

    sweep(rhs, fields, cols, count, one)
    sweep(mid, fields, cols, count, two)


def keep(f, j, v, u):
    return u


def repeat(count, body):
    def one(k, carry):
        body(k)
        return carry

    lax.fori_loop(0, count, one, 0)


def turn(dst, ref):
    for h in range(2):
        for b in range(2):
            block = ref[128 * b : 128 * b + 128, 128 * h : 128 * h + 128]
            dst[b, HALO + 128 * h : HALO + 128 * h + 128, :] = block.T


def turn_edge(dst, above, below, edge):
    for h in range(2):
        cols = slice(128 * h, 128 * h + 128)
        edge[0:HALO, :] = below[:, cols]
        edge[128 - HALO : 128, :] = above[:, cols]
        dst[2, HALO + 128 * h : HALO + 128 * h + 128, :] = edge[...].T


def lay(dst, turned, line):
    pad = jnp.zeros((128 - LIVE, 128), F32)
    for j in range(3):
        for b in range(3):
            got = jnp.concatenate([turned[b, pl.ds(j, LIVE, stride=3), :], pad], axis=0).T
            if b < 2:
                line[HALO + 128 * b : HALO + 128 * b + 128, :] = got
            else:
                line[HALO + N : EXT, :] = got[0:HALO, :]
                line[0:HALO, :] = got[128 - HALO : 128, :]
        mix(dst.at[j], natural(line, V), V)


def unlay(write, read, line, turned):
    for j in range(3):
        unmix(line, lambda v: read(j, v), V)
        for b in range(2):
            got = line[HALO + 128 * b : HALO + 128 * b + 128, :].T
            turned[b, pl.ds(j, LIVE, stride=3), :] = got[0:LIVE, :]
    for b in range(2):
        for h in range(2):
            write(b, h, turned[b, HALO + 128 * h : HALO + 128 * h + 128, :].T)


def restrict(ref, f, pair):
    lane = lax.broadcasted_iota(jnp.int32, (128, C), 0)
    coarse = lax.broadcasted_iota(jnp.int32, (128, C), 1)
    out = None
    for j in range(3):
        for i in range(HV):
            pair[vec(i), :] = ref[f, j, vec(2 * i), :] + ref[f, j, vec(2 * i + 1), :]
        pick = jnp.where((3 * lane + j) // 2 - 8 == coarse, 0.25, 0.0).astype(F32)
        part = jnp.dot(pair[...], pick, precision=lax.Precision.HIGHEST, preferred_element_type=F32)
        out = part if out is None else out + part
    return out


def strips_body(source, iterate, start, conduct, up, down, last, sems):
    is_end = lax.axis_index("tm") == lax.axis_size("tm") - 1
    low, high = pl.ds(0, HALO), pl.ds(N - HALO, HALO)
    copies = []
    for ref, rows in ((up, low), (down, high)):
        copies.append((source.at[:, rows, :], ref.at[pl.ds(0, 8)]))
        copies.append((iterate.at[3, rows, :], ref.at[MID]))
        copies.append((conduct.at[rows, :], ref.at[COEF]))
    copies = [pltpu.make_async_copy(a, b, sems.at[i]) for i, (a, b) in enumerate(copies)]
    for c in copies:
        c.start()

    @pl.when(is_end)
    def _():
        c = pltpu.make_async_copy(start, last, sems.at[6])
        c.start()
        c.wait()

    @pl.when(jnp.logical_not(is_end))
    def _():
        c = pltpu.make_async_copy(iterate.at[7], last, sems.at[6])
        c.start()
        c.wait()

    up[LAST] = last[0:HALO, :]
    down[LAST] = last[N - HALO : N, :]
    for c in copies:
        c.wait()


def pack_edges(pieces, rows):
    lane = lanes(rows)
    low = [jnp.zeros((rows, 128), F32) for _ in range((len(pieces) + 7) // 8)]
    high = list(low)
    for f, (head, tail) in enumerate(pieces):
        at, k = HALO * (f % 8), f // 8
        inside = (lane >= at) & (lane < at + HALO)
        low[k] = jnp.where(inside, roll(head, at), low[k])
        high[k] = jnp.where(inside, roll(tail, at + HALO), high[k])
    return low, high


def center_body(source, iterate, last, conduct, turned, low, high, src, middle, coef, sems):
    pairs = ((source, src), (iterate.at[3], middle), (conduct, coef))
    copies = [pltpu.make_async_copy(a, b, sems.at[i]) for i, (a, b) in enumerate(pairs)]
    for c in copies:
        c.start()
    for c in copies:
        c.wait()
    for f, ref in enumerate([src.at[f] for f in range(8)] + [middle, last, coef]):
        turn(turned.at[f], ref)
        for b in range(2):
            at = slice(HALO * f, HALO * f + HALO)
            low[b, at, :] = turned[f, b, HALO : 2 * HALO, :]
            high[b, at, :] = turned[f, b, N : N + HALO, :]


def rows_body(turned_in, above, below, turned, low, high, top, bottom, edge):
    del turned_in
    place, ends = lax.axis_index("sx"), lax.axis_size("sx") - 1
    up, down = flag(place > 0), flag(place < ends)
    edge[...] = jnp.zeros((128, 128), F32)
    lane = lanes(HALO)
    out = {}
    for f in range(FIELDS):
        top[...] = above[f] * up
        bottom[...] = below[f] * down
        turn_edge(turned.at[f], top, bottom, edge)
        at = 2 * HALO * (f // 3)
        for k, base in ((0, HALO), (1, N)):
            x = roll(turned[f, 2, base : base + HALO, :], HALO + at)
            old = out.get((k, f % 3), jnp.zeros((HALO, 128), F32))
            out[k, f % 3] = jnp.where((lane >= at) & (lane < at + 2 * HALO), x, old)
    for i in range(3):
        low[HALO * i : HALO * i + HALO, :] = out[0, i]
        high[HALO * i : HALO * i + HALO, :] = out[1, i]


def side_column(before, after, f, rows, first, final):
    lane = lanes(rows)
    at = HALO * (f % 8)
    right = jnp.where(lane < HALO, roll(after, -at) * final, 0.0)
    return jnp.where(lane >= 128 - HALO, roll(before, -HALO - at) * first, right)


QUARTER = EXT // 4
PART1 = 2 * EXT + QUARTER
PART2 = PART1 + 4 * HALO
MAIN = PART2 + 6 * HALO


def squeeze(dest, ref):
    lane = lanes(8)
    for v in range(V):
        third = ref[2, vec(v), :]
        dest[8 * v : 8 * v + 8, :] = jnp.where(lane < LIVE, ref[0, vec(v), :], roll(third, 96))
        dest[EXT + 8 * v : EXT + 8 * v + 8, :] = jnp.where(lane < LIVE, ref[1, vec(v), :], roll(third, 64))
    for i in range(QUARTER // 8):
        out = None
        for g in range(4):
            x = roll(ref[2, vec(i + g * QUARTER // 8), :], 32 * g - 64)
            out = x if out is None else jnp.where(lane >= 32 * g, x, out)
        dest[2 * EXT + 8 * i : 2 * EXT + 8 * i + 8, :] = out


def unsqueeze(dest, src):
    lane = lanes(8)
    for v in range(V):
        a, b = src[8 * v : 8 * v + 8, :], src[EXT + 8 * v : EXT + 8 * v + 8, :]
        dest[0, vec(v), :] = jnp.where(lane < LIVE, a, 0.0)
        dest[1, vec(v), :] = jnp.where(lane < LIVE, b, 0.0)
        g, i = divmod(v, QUARTER // 8)
        rest = roll(src[2 * EXT + 8 * i : 2 * EXT + 8 * i + 8, :], 64 - 32 * g)
        third = jnp.where(lane < 32, roll(a, 32), jnp.where(lane < 64, roll(b, 64), rest))
        dest[2, vec(v), :] = jnp.where(lane < LIVE, third, 0.0)


def fold(dest, base, columns, width, groups, rows_in):
    span = 2 * width
    rows = rows_in // groups
    lane = lanes(rows)
    out = jnp.zeros((rows, 128), F32)
    for g in range(groups):
        for k, read in enumerate(columns):
            at = (g * len(columns) + k) * span
            inside = (lane >= at) & (lane < at + span)
            out = jnp.where(inside, roll(read(g * rows, rows), width + at), out)
    dest[base : base + rows, :] = out


def unfold(src, base, k, count, width, groups, rows_in, write):
    span = 2 * width
    rows = rows_in // groups
    lane = lanes(rows)
    for g in range(groups):
        at = (g * count + k) * span
        x = roll(src[base : base + rows, :], -width - at)
        write(g * rows, rows, jnp.where((lane < width) | (lane >= 128 - width), x, 0.0))


def local_body(
    turned_in, above, below, before, after, before_c, after_c,
    turned, ext, coefs, forced, own_new, main, up, down, low_c, high_c, coarse,
    rhs, mid, scaled, line, pair, rows_c,
):
    del turned_in
    t, x, z = lax.axis_index("tm"), lax.axis_index("sx"), lax.axis_index("sy")
    not_end = flag(t < lax.axis_size("tm") - 1)
    x_first, x_final = flag(x > 0), flag(x < lax.axis_size("sx") - 1)
    z_first, z_final = flag(z > 0), flag(z < lax.axis_size("sy") - 1)
    inv, cof = coefs.at[0], coefs.at[1]
    lane = lanes(HALO)
    ends = (lane < HALO) | (lane >= 128 - HALO)
    for f in range(FIELDS):
        for own, corner, base, present in ((before, before_c, 0, z_first), (after, after_c, HALO + N, z_final)):
            for b in range(2):
                turned[f, b, base : base + HALO, :] = own[b, HALO * f : HALO * f + HALO, :] * present
            x = roll(corner[HALO * (f % 3) : HALO * (f % 3) + HALO, :], -HALO - 2 * HALO * (f // 3))
            turned[f, 2, base : base + HALO, :] = jnp.where(ends, x * present, 0.0)

    def lay_field(f):
        lay(ext.at[f], turned.at[f], line)

    repeat(FIELDS, lay_field)
    for v in range(V):
        for j in range(3):
            c = ext[COEF, j, vec(v), :]
            r = 1.0 / (1.0 + 4.0 * c)
            inv[j, vec(v), :] = r
            cof[j, vec(v), :] = c * r
            rhs[0, j, vec(v), :] = ext[MID, j, vec(v), :] + ext[4, j, vec(v), :]
            rhs[1, j, vec(v), :] = ext[0, j, vec(v), :]
            rhs[2, j, vec(v), :] = ext[LAST, j, vec(v), :]

    def forced_step(k):
        def add(f, j, v, u):
            return u if f == 2 else u + ext[(5 if f == 0 else 1) + k, j, vec(v), :]

        step(rhs, mid, scaled, inv, cof, range(3), 3, V, add)

    repeat(FACTOR - 1, forced_step)

    def between():
        for v in range(V):
            for j in range(3):
                new, old = rhs[0, j, vec(v), :], ext[LAST, j, vec(v), :]
                moved = not_end * (new - old)
                own_new[j, vec(v), :] = new
                scaled[0, j, vec(v), :] = old + moved
                rhs[0, j, vec(v), :] = moved
                s = rhs[1, j, vec(v), :]
                forced[j, vec(v), :] = s
                rhs[1, j, vec(v), :] = s - ext[MID, j, vec(v), :]
        squeeze(main, scaled.at[0])
        for j in range(2):
            cols = slice(128 * j, 128 * j + 128)
            at = PART1 + 2 * HALO * j
            main[at : at + HALO, :] = above[LAST, :, cols] * x_first
            main[at + HALO : at + 2 * HALO, :] = below[LAST, :, cols] * x_final
        for b in range(3):
            at = PART2 + 2 * HALO * b
            main[at : at + HALO, :] = turned[LAST, b, 0:HALO, :]
            main[at + HALO : at + 2 * HALO, :] = turned[LAST, b, HALO + N : EXT, :]

    def free_step(k):
        step(rhs, mid, scaled, inv, cof, range(3), 3, V, keep)
        pl.when(k == 0)(between)

    repeat(FACTOR + 1, free_step)
    for k, (ref, f) in enumerate(((rhs, 1), (rhs, 0), (rhs, 2), (ext, COEF))):
        got = restrict(ref, f, pair)
        pair[...] = got
        unmix(rows_c, lambda v: pair[vec(v), :], HV)
        coarse[k] = rows_c[8 : 8 + C, :]
    for k in range(4):
        up[k] = coarse[k, 0:HALO, :]
        down[k] = coarse[k, C - HALO : C, :]
    lo, hi = pack_edges([(coarse[k], coarse[k]) for k in range(4)], C)
    low_c[...] = lo[0]
    high_c[...] = hi[0]


def coarse_edges_body(above, below, low_c, high_c, low, high):
    place, ends = lax.axis_index("sx"), lax.axis_size("sx") - 1
    low[HALO : HALO + C, :] = low_c[...]
    high[HALO : HALO + C, :] = high_c[...]
    for ref, base, present in ((above, 0, flag(place > 0)), (below, HALO + C, flag(place < ends))):
        lo, hi = pack_edges([(ref[k] * present,) * 2 for k in range(4)], HALO)
        low[base : base + HALO, :] = lo[0]
        high[base : base + HALO, :] = hi[0]


ONE = 2 * CEXT + CEXT // 4
TWO = CEXT + CEXT // 5


def coarse_body(coarse, above, below, before, after, one, two, three, four, coefs, ext, rhs, mid, scaled, wide):
    t, x, z = lax.axis_index("tm"), lax.axis_index("sx"), lax.axis_index("sy")
    not_end = flag(t < lax.axis_size("tm") - 1)
    x_first, x_final = flag(x > 0), flag(x < lax.axis_size("sx") - 1)
    z_first, z_final = flag(z > 0), flag(z < lax.axis_size("sy") - 1)
    for k in range(4):
        wide[0:HALO, :] = above[k] * x_first
        wide[HALO : HALO + C, :] = coarse[k]
        wide[HALO + C : CEXT, :] = below[k] * x_final
        mix(ext.at[k, 0], natural(wide, CV), CV)
    for v in range(CV):
        left, right = natural(before, CV)(v), natural(after, CV)(v)
        for k in range(4):
            ext[k, 1, vec(v), :] = side_column(left, right, k, 8, z_first, z_final)
    inv, cof = coefs.at[0], coefs.at[1]
    for j in range(2):
        c = ext[3, j]
        r = 1.0 / (1.0 + 4.0 * c)
        inv[j] = r
        cof[j] = c * r
        rhs[0, j] = ext[0, j] * not_end
        rhs[1, j] = ext[1, j]

    def advance(fields, after_step):
        step(rhs, mid, scaled, inv, cof, fields, 2, CV, after_step)

    def reader(ref, f):
        return lambda r, n: ref[f, 1, r : r + n, :]

    one[0:CEXT, :] = ext[0, 0]
    one[CEXT : 2 * CEXT, :] = ext[1, 0]
    fold(one, 2 * CEXT, [reader(ext, 0), reader(ext, 1)], 8, 4, CEXT)
    advance(range(2), lambda f, j, v, u: u if f == 0 else u + ext[2, j, vec(v), :])
    for j in range(2):
        ext[2, j] = rhs[1, j]
    advance(range(2), lambda f, j, v, u: u + ext[2, j, vec(v), :] if f == 0 else u)
    two[0:CEXT, :] = rhs[0, 0]
    fold(two, CEXT, [reader(rhs, 0)], 8, 5, CEXT)
    repeat(2, lambda k: advance(range(2), keep))
    three[0:CEXT, :] = rhs[0, 0]
    fold(three, CEXT, [reader(rhs, 0)], 8, 5, CEXT)
    advance(range(1, 2), keep)
    for j in range(2):
        four[j] = rhs[1, j]


def arrive_body(
    last, main, ext, coefs, forced, resid, new_start, new_mid, coarse_mid,
    rhs, mid, scaled, turned, top, bottom, edge, line, pair,
):
    inv, cof = coefs.at[0], coefs.at[1]
    edge[...] = jnp.zeros((128, 128), F32)
    for j in range(2):
        at, cols = PART1 + 2 * HALO * j, slice(128 * j, 128 * j + 128)
        top[:, cols] = main[at : at + HALO, :]
        bottom[:, cols] = main[at + HALO : at + 2 * HALO, :]
    for b in range(3):
        at = PART2 + 2 * HALO * b
        turned[b, 0:HALO, :] = main[at : at + HALO, :]
        turned[b, HALO + N : EXT, :] = main[at + HALO : at + 2 * HALO, :]
    turn(turned, last)
    turn_edge(turned, top, bottom, edge)
    lay(rhs.at[0], turned, line)
    unsqueeze(new_start, main)
    for j in range(3):
        rhs[1, j] = new_start[j] - rhs[0, j]
    repeat(FACTOR, lambda k: step(rhs, mid, scaled, inv, cof, range(2), 3, V, keep))
    for j in range(3):
        for v in range(V):
            u = rhs[0, j, vec(v), :] + forced[j, vec(v), :]
            new_mid[j, vec(v), :] = u
            rhs[0, j, vec(v), :] = u - ext[MID, j, vec(v), :]
    repeat(FACTOR, lambda k: step(rhs, mid, scaled, inv, cof, range(1), 3, V, keep))
    for k in range(2):

        def put(b, h, block, k=k):
            resid[k, 128 * b : 128 * b + 128, 128 * h : 128 * h + 128] = block

        unlay(put, lambda j, v, k=k: rhs[1 - k, j, vec(v), :], line, turned)
    coarse_mid[...] = restrict(rhs, 0, pair)


def final_body(
    one, two, three, four, ccoefs, coarse_mid, ext, coefs, new_start, new_mid, own_new,
    out, err, cmid, cscaled, sent, fix, rhs, mid, scaled, turned, line, pair, rows_c,
):
    t = lax.axis_index("tm")
    m1, m2, m3 = flag(t > 0), flag(t > 1), flag(t > 2)
    inv, cof = ccoefs.at[0], ccoefs.at[1]

    def put(k):
        def write(r, n, value):
            sent[k, r : r + n, :] = value

        return write

    unfold(one, 2 * CEXT, 0, 2, 8, 4, CEXT, put(0))
    unfold(one, 2 * CEXT, 1, 2, 8, 4, CEXT, put(1))
    unfold(two, CEXT, 0, 1, 8, 5, CEXT, put(2))
    unfold(three, CEXT, 0, 1, 8, 5, CEXT, put(3))
    err[0, 0] = m1 * (one[0:CEXT, :] + two[0:CEXT, :]) + m2 * three[0:CEXT, :] + m3 * four[0]
    err[0, 1] = m1 * (sent[0] + sent[2]) + m2 * sent[3] + m3 * four[1]

    def spread(k, extra=None):
        src = lax.broadcasted_iota(jnp.int32, (128, 128), 0)
        dst = lax.broadcasted_iota(jnp.int32, (128, 128), 1)
        for c in range(2 if extra is None else 1):
            unmix(rows_c, lambda v: err[0, c, vec(v), :], CV)
            mix(pair, natural(rows_c, HV, 8), HV)
            value = pair[...] if extra is None else pair[...] + extra[...]
            for j in range(3):
                cell = (3 * dst + j) // 2 - 8
                if c == 1:
                    cell = jnp.where(cell < 0, cell + C, jnp.where((cell >= C) & (dst < LIVE), cell - C, -1))
                got = jnp.dot(value, flag(src == cell), precision=lax.Precision.HIGHEST, preferred_element_type=F32)
                fix[k, j] = got if c == 0 else fix[k, j] + got

    spread(0)
    step(err, cmid, cscaled, inv, cof, range(1), 2, CV, keep)
    err[0, 0] += one[CEXT : 2 * CEXT, :]
    err[0, 1] += sent[1]
    spread(1)
    step(err, cmid, cscaled, inv, cof, range(1), 2, CV, keep)
    spread(2, coarse_mid)
    inv, cof = coefs.at[0], coefs.at[1]
    for v in range(V):
        for j in range(3):
            rhs[0, j, vec(v), :] = new_start[j, vec(v), :] + fix[0, j, vec(v // 2), :] + ext[0, j, vec(v), :]
            u = new_mid[j, vec(v), :] + fix[1, j, vec(v // 2), :]
            scaled[0, j, vec(v), :] = u
            rhs[1, j, vec(v), :] = u + ext[4, j, vec(v), :]
            scaled[1, j, vec(v), :] = own_new[j, vec(v), :] + fix[2, j, vec(v // 2), :]

    def give(at):
        for f in range(2):

            def put(b, h, block, f=f):
                out[4 * f + at, 128 * b : 128 * b + 128, 128 * h : 128 * h + 128] = block

            unlay(put, lambda j, v, f=f: scaled[f, j, vec(v), :], line, turned)

    give(FACTOR - 1)

    def fine(k):
        def add(f, j, v, u):
            scaled[f, j, vec(v), :] = u
            return u + ext[4 * f + 1 + k, j, vec(v), :]

        step(rhs, mid, scaled, inv, cof, range(2), 3, V, add)
        give(k)

    repeat(FACTOR - 1, fine)


def ring(x, axis, by):
    count = lax.axis_size(axis)
    return lax.ppermute(x, axis, [(i, (i + by) % count) for i in range(count)])


def vmem(*shape):
    return pltpu.VMEM(shape, F32)


def shards(iterate, source, start_field, conduct):
    up, down, last = call(
        strips_body, [(FIELDS, HALO, N)] * 2 + [(N, N)], [HB] * 4, [pltpu.SemaphoreType.DMA((7,))], name="strips",
        limit=63_000_000,
    )(source, iterate, start_field, conduct)
    above, below = ring(down, "sx", 1), ring(up, "sx", -1)
    last_in = ring(last, "tm", 1)
    turned, low, high = call(
        center_body,
        [(FIELDS, 3, EXT, 128), (2, HALO * FIELDS, 128), (2, HALO * FIELDS, 128)],
        [HB, HB, VM, HB],
        [vmem(8, N, N), vmem(N, N), vmem(N, N), pltpu.SemaphoreType.DMA((3,))],
        name="center", flops=20_000_000,
    )(source, iterate, last, conduct)
    before, after = ring(high, "sy", 1), ring(low, "sy", -1)
    turned, c_lo, c_hi = call(
        rows_body, [(FIELDS, 3, EXT, 128), (3 * HALO, 128), (3 * HALO, 128)], 3,
        [vmem(HALO, N), vmem(HALO, N), vmem(128, 128)], {0: 0}, "rows",
    )(turned, above, below)
    before_c, after_c = ring(c_hi, "sy", 1), ring(c_lo, "sy", -1)
    before, after, before_c, after_c, last_in = lax.optimization_barrier((before, after, before_c, after_c, last_in))
    _, ext, coefs, forced, own_new, main, c_up, c_down, c_low, c_high, coarse = call(
        local_body,
        [
            (FIELDS, 3, EXT, 128), (FIELDS, 3, EXT, 128), (2, 3, EXT, 128), (3, EXT, 128), (3, EXT, 128), (MAIN, 128),
            (4, HALO, 128), (4, HALO, 128), (C, 128), (C, 128), (4, C, 128),
        ],
        7, [vmem(3, 3, EXT, 128)] * 3 + [vmem(EXT, 128), vmem(HALF, 128), vmem(HALF, 128)],
        {0: 0}, "local", 50_000_000,
    )(turned, above, below, before, after, before_c, after_c)
    c_above, c_below = ring(c_down, "sx", 1), ring(c_up, "sx", -1)
    main_in = ring(main, "tm", 1)
    c_lo, c_hi = call(coarse_edges_body, [(CEXT, 128)] * 2, 4, name="coarse_edges")(c_above, c_below, c_low, c_high)
    c_before, c_after = ring(c_hi, "sy", 1), ring(c_lo, "sy", -1)
    one, two, three, four, ccoefs = call(
        coarse_body,
        [(ONE, 128), (TWO, 128), (TWO, 128), (2, CEXT, 128), (2, 2, CEXT, 128)],
        5,
        [vmem(4, 2, CEXT, 128)] + [vmem(2, 2, CEXT, 128)] * 3 + [vmem(CEXT, 128)],
        name="coarse",
    )(coarse, c_above, c_below, c_before, c_after)
    one, two, three = ring(one, "tm", 1), ring(two, "tm", 2), ring(three, "tm", 3)
    resid, new_start, new_mid, coarse_mid = call(
        arrive_body,
        [(2, N, N), (3, EXT, 128), (3, EXT, 128), (HALF, 128)],
        5,
        [vmem(2, 3, EXT, 128)] * 3
        + [vmem(3, EXT, 128), vmem(HALO, N), vmem(HALO, N), vmem(128, 128), vmem(EXT, 128), vmem(HALF, 128)],
        name="arrive", flops=30_000_000,
    )(last_in, main_in, ext, coefs, forced)
    (updated,) = call(
        final_body,
        [(8, N, N)],
        11,
        [vmem(1, 2, CEXT, 128)] * 3 + [vmem(4, CEXT, 128), vmem(3, 3, HALF, 128)] + [vmem(2, 3, EXT, 128)] * 3
        + [vmem(2, EXT, 128), vmem(EXT, 128), vmem(HALF, 128), vmem(CEXT, 128)],
        name="final",
    )(one, two, three, four, ccoefs, coarse_mid, ext, coefs, new_start, new_mid, own_new)
    return updated, resid


def solution(mesh):
    in_specs = (P("tm", "sx", "sy"), P("tm", "sx", "sy"), P("sx", "sy"), P("sx", "sy"))
    out_specs = (P("tm", "sx", "sy"), P("tm", "sx", "sy"))
    return jax.shard_map(shards, mesh=mesh, in_specs=in_specs, out_specs=out_specs, check_vma=False)
```

```python
import jax
import jax.numpy as jnp
from jax import lax
from jax.experimental import pallas as pl
from jax.experimental.pallas import tpu as pltpu
from jax.sharding import PartitionSpec as P


FACTOR = 4
N = 256
HALO = 16
EXT = N + 2 * HALO
V = EXT // 8
C = N // 2
CEXT = C + 2 * HALO
CV = CEXT // 8
HALF = EXT // 2
HV = HALF // 8
FIELDS = 11
MID, LAST, COEF = 8, 9, 10
LIVE = EXT // 3
F32 = jnp.float32
LIMIT = 24 * 1024 * 1024

VM = pl.BlockSpec(memory_space=pltpu.VMEM)
HB = pl.BlockSpec(memory_space=pltpu.HBM)


def call(body, outs, ins, scratch=(), aliases=None, flops=0, limit=LIMIT, out_specs=None):
    return pl.pallas_call(
        body,
        out_shape=[jax.ShapeDtypeStruct(s, F32) for s in outs],
        in_specs=[VM] * ins if isinstance(ins, int) else ins,
        out_specs=out_specs or [VM] * len(outs),
        scratch_shapes=list(scratch),
        input_output_aliases=aliases or {},
        compiler_params=pltpu.CompilerParams(vmem_limit_bytes=limit),
        cost_estimate=pl.CostEstimate(flops=flops, bytes_accessed=1000, transcendentals=0),
    )


def lanes(rows):
    return lax.broadcasted_iota(jnp.int32, (rows, 128), 1)


def roll(x, by):
    by %= 128
    return pltpu.roll(x, by, 1) if by else x


def flag(condition):
    return jnp.where(condition, 1.0, 0.0).astype(F32)


def vec(v):
    return slice(8 * v, 8 * v + 8)


def mix(dest, read, count):
    for v in range(count):
        dest[vec(v), :] = read(v)


def natural(ref, count, offset=0):
    return lambda v: ref[pl.ds(offset + v, 8, stride=count), :]


def unmix(dest, read, count):
    for v in range(count):
        dest[pl.ds(v, 8, stride=count), :] = read(v)


def sweep(src, edge, fields, cols, count, emit):
    lane = lanes(8)
    first, last = lane == 0, lane == 127
    held = {}

    def at(f, j, v):
        if (f, j, v) not in held:
            held[f, j, v] = src[f, j, vec(v), :]
        return held[f, j, v]

    for v in range(count):
        for f in fields:
            mid = [at(f, j, v) for j in range(cols)]
            if cols == 3:
                ends = None if edge is None else (edge[f, 0, vec(v), :], edge[f, 1, vec(v), :])
                ends = ends or (pltpu.roll(mid[2], 1, 1), pltpu.roll(mid[0], 127, 1))
                left, right = [ends[0], mid[0], mid[1]], [mid[1], mid[2], ends[1]]
            else:
                back = [pltpu.roll(m, 1, 1) for m in mid]
                ahead = [pltpu.roll(m, 127, 1) for m in mid]
                left = [jnp.where(first, back[1 - j], back[j]) for j in range(2)]
                right = [jnp.where(last, ahead[1 - j], ahead[j]) for j in range(2)]
            for j in range(cols):
                below = at(f, j, v + 1) if v + 1 < count else pltpu.roll(src[f, j, vec(0), :], 7, 0)
                above = at(f, j, v - 1) if v else pltpu.roll(src[f, j, vec(count - 1), :], 1, 0)
                emit(f, j, v, mid[j], (below + above) + (left[j] + right[j]))
        for key in [k for k in held if k[2] < v]:
            del held[key]


def put_edge(edge, f, j, v, x):
    if edge is not None and j == 2:
        edge[f, 0, vec(v), :] = pltpu.roll(x, 1, 1)
    if edge is not None and j == 0:
        edge[f, 1, vec(v), :] = pltpu.roll(x, 127, 1)


def step(rhs, mid, scaled, inv, cof, fields, cols, count, after, edges=(None, None)):
    def one(f, j, v, own, total):
        b = own * inv[j, vec(v), :]
        scaled[f, j, vec(v), :] = b
        w = b + cof[j, vec(v), :] * total
        mid[f, j, vec(v), :] = w
        put_edge(edges[1], f, j, v, w)

    def two(f, j, v, own, total):
        u = scaled[f, j, vec(v), :] + cof[j, vec(v), :] * total
        b = after(f, j, v, u)
        rhs[f, j, vec(v), :] = b
        put_edge(edges[0], f, j, v, b)

    sweep(rhs, edges[0], fields, cols, count, one)
    sweep(mid, edges[1], fields, cols, count, two)


def put_edges(edge, rhs, fields):
    for f in fields:
        for v in range(V):
            for j in (0, 2):
                put_edge(edge, f, j, v, rhs[f, j, vec(v), :])


def keep(f, j, v, u):
    return u


def repeat(count, body):
    def one(k, carry):
        body(k)
        return carry

    lax.fori_loop(0, count, one, 0)


def turn(dst, ref):
    for h in range(2):
        for b in range(2):
            block = ref[128 * b : 128 * b + 128, 128 * h : 128 * h + 128]
            dst[b, HALO + 128 * h : HALO + 128 * h + 128, :] = block.T


def turn_edge(dst, above, below, edge):
    for h in range(2):
        cols = slice(128 * h, 128 * h + 128)
        edge[0:HALO, :] = below[:, cols]
        edge[128 - HALO : 128, :] = above[:, cols]
        dst[2, HALO + 128 * h : HALO + 128 * h + 128, :] = edge[...].T


def lay(dst, turned, line):
    pad = jnp.zeros((128 - LIVE, 128), F32)
    for j in range(3):
        for b in range(3):
            got = jnp.concatenate([turned[b, pl.ds(j, LIVE, stride=3), :], pad], axis=0).T
            if b < 2:
                line[HALO + 128 * b : HALO + 128 * b + 128, :] = got
            else:
                line[HALO + N : EXT, :] = got[0:HALO, :]
                line[0:HALO, :] = got[128 - HALO : 128, :]
        mix(dst.at[j], natural(line, V), V)


def unlay(write, read, line, turned):
    for j in range(3):
        unmix(line, lambda v: read(j, v), V)
        for b in range(2):
            got = line[HALO + 128 * b : HALO + 128 * b + 128, :].T
            turned[b, pl.ds(j, LIVE, stride=3), :] = got[0:LIVE, :]
    for b in range(2):
        for h in range(2):
            write(b, h, turned[b, HALO + 128 * h : HALO + 128 * h + 128, :].T)


def select(x, pick):
    high = x.astype(jnp.bfloat16)
    rest = x - high.astype(F32)
    mid = rest.astype(jnp.bfloat16)
    low = (rest - mid.astype(F32)).astype(jnp.bfloat16)
    parts = [jnp.dot(p, pick, preferred_element_type=F32) for p in (low, mid, high)]
    return (parts[0] + parts[1]) + parts[2]


def restrict(ref, f, pair):
    lane = lax.broadcasted_iota(jnp.int32, (3 * 128, C), 0)
    coarse = lax.broadcasted_iota(jnp.int32, (3 * 128, C), 1)
    column = 3 * (lane % 128) + lane // 128
    pick = jnp.where(column // 2 - 8 == coarse, 0.25, 0.0).astype(jnp.bfloat16)
    for j in range(3):
        for i in range(HV):
            pair[vec(i), 128 * j : 128 * j + 128] = ref[f, j, vec(2 * i), :] + ref[f, j, vec(2 * i + 1), :]
    return select(pair[...], pick)


def load_body(source, iterate, start, conduct, up, down, src, middle, last, coef, sems):
    is_end = lax.axis_index("tm") == lax.axis_size("tm") - 1
    pairs = ((source, src), (iterate.at[3], middle), (conduct, coef))
    copies = [pltpu.make_async_copy(a, b, sems.at[i]) for i, (a, b) in enumerate(pairs)]
    for c in copies:
        c.start()

    @pl.when(is_end)
    def _():
        c = pltpu.make_async_copy(start, last, sems.at[3])
        c.start()
        c.wait()

    @pl.when(jnp.logical_not(is_end))
    def _():
        c = pltpu.make_async_copy(iterate.at[7], last, sems.at[3])
        c.start()
        c.wait()

    for c in copies:
        c.wait()
    for f, ref in enumerate([src.at[f] for f in range(8)] + [middle, last, coef]):
        up[f] = ref[0:HALO, :]
        down[f] = ref[N - HALO : N, :]


def pack_edges(pieces, rows):
    lane = lanes(rows)
    low = [jnp.zeros((rows, 128), F32) for _ in range((len(pieces) + 7) // 8)]
    high = list(low)
    for f, (head, tail) in enumerate(pieces):
        at, k = HALO * (f % 8), f // 8
        inside = (lane >= at) & (lane < at + HALO)
        low[k] = jnp.where(inside, roll(head, at), low[k])
        high[k] = jnp.where(inside, roll(tail, at + HALO), high[k])
    return low, high


def center_body(src, middle, last, coef, turned, low, high):
    for f, ref in enumerate([src.at[f] for f in range(8)] + [middle, last, coef]):
        turn(turned.at[f], ref)
        for b in range(2):
            at = slice(HALO * f, HALO * f + HALO)
            low[b, at, :] = turned[f, b, HALO : 2 * HALO, :]
            high[b, at, :] = turned[f, b, N : N + HALO, :]


def rows_body(turned_in, above, below, turned, low, high, top, bottom, edge):
    del turned_in
    place, ends = lax.axis_index("sx"), lax.axis_size("sx") - 1
    up, down = flag(place > 0), flag(place < ends)
    edge[...] = jnp.zeros((128, 128), F32)
    lane = lanes(HALO)
    out = {}
    for f in range(FIELDS):
        top[...] = above[f] * up
        bottom[...] = below[f] * down
        turn_edge(turned.at[f], top, bottom, edge)
        at = 2 * HALO * (f // 3)
        for k, base in ((0, HALO), (1, N)):
            x = roll(turned[f, 2, base : base + HALO, :], HALO + at)
            old = out.get((k, f % 3), jnp.zeros((HALO, 128), F32))
            out[k, f % 3] = jnp.where((lane >= at) & (lane < at + 2 * HALO), x, old)
    for i in range(3):
        low[HALO * i : HALO * i + HALO, :] = out[0, i]
        high[HALO * i : HALO * i + HALO, :] = out[1, i]


def side_column(before, after, f, rows, first, final):
    lane = lanes(rows)
    at = HALO * (f % 8)
    right = jnp.where(lane < HALO, roll(after, -at) * final, 0.0)
    return jnp.where(lane >= 128 - HALO, roll(before, -HALO - at) * first, right)


QUARTER = EXT // 4
PART1 = 2 * EXT + QUARTER
PART2 = PART1 + 4 * HALO
MAIN = PART2 + 6 * HALO


def squeeze(dest, ref):
    lane = lanes(8)
    for v in range(V):
        third = ref[2, vec(v), :]
        dest[8 * v : 8 * v + 8, :] = jnp.where(lane < LIVE, ref[0, vec(v), :], roll(third, 96))
        dest[EXT + 8 * v : EXT + 8 * v + 8, :] = jnp.where(lane < LIVE, ref[1, vec(v), :], roll(third, 64))
    for i in range(QUARTER // 8):
        out = None
        for g in range(4):
            x = roll(ref[2, vec(i + g * QUARTER // 8), :], 32 * g - 64)
            out = x if out is None else jnp.where(lane >= 32 * g, x, out)
        dest[2 * EXT + 8 * i : 2 * EXT + 8 * i + 8, :] = out


def unsqueeze(dest, src):
    lane = lanes(8)
    for v in range(V):
        a, b = src[8 * v : 8 * v + 8, :], src[EXT + 8 * v : EXT + 8 * v + 8, :]
        dest[0, vec(v), :] = jnp.where(lane < LIVE, a, 0.0)
        dest[1, vec(v), :] = jnp.where(lane < LIVE, b, 0.0)
        g, i = divmod(v, QUARTER // 8)
        rest = roll(src[2 * EXT + 8 * i : 2 * EXT + 8 * i + 8, :], 64 - 32 * g)
        third = jnp.where(lane < 32, roll(a, 32), jnp.where(lane < 64, roll(b, 64), rest))
        dest[2, vec(v), :] = jnp.where(lane < LIVE, third, 0.0)


def fold(dest, base, columns, width, groups, rows_in):
    span = 2 * width
    rows = rows_in // groups
    lane = lanes(rows)
    out = jnp.zeros((rows, 128), F32)
    for g in range(groups):
        for k, read in enumerate(columns):
            at = (g * len(columns) + k) * span
            inside = (lane >= at) & (lane < at + span)
            out = jnp.where(inside, roll(read(g * rows, rows), width + at), out)
    dest[base : base + rows, :] = out


def unfold(src, base, k, count, width, groups, rows_in, write):
    span = 2 * width
    rows = rows_in // groups
    lane = lanes(rows)
    for g in range(groups):
        at = (g * count + k) * span
        x = roll(src[base : base + rows, :], -width - at)
        write(g * rows, rows, jnp.where((lane < width) | (lane >= 128 - width), x, 0.0))


def local_body(
    turned_in, above, below, before, after, before_c, after_c,
    turned, ext, coefs, forced, own_new, main, up, down, low_c, high_c, coarse,
    rhs, mid, scaled, line, pair, rows_c, *edges,
):
    del turned_in
    t, x, z = lax.axis_index("tm"), lax.axis_index("sx"), lax.axis_index("sy")
    not_end = flag(t < lax.axis_size("tm") - 1)
    x_first, x_final = flag(x > 0), flag(x < lax.axis_size("sx") - 1)
    z_first, z_final = flag(z > 0), flag(z < lax.axis_size("sy") - 1)
    inv, cof = coefs.at[0], coefs.at[1]
    lane = lanes(HALO)
    ends = (lane < HALO) | (lane >= 128 - HALO)
    for f in range(FIELDS):
        for own, corner, base, present in ((before, before_c, 0, z_first), (after, after_c, HALO + N, z_final)):
            for b in range(2):
                turned[f, b, base : base + HALO, :] = own[b, HALO * f : HALO * f + HALO, :] * present
            x = roll(corner[HALO * (f % 3) : HALO * (f % 3) + HALO, :], -HALO - 2 * HALO * (f // 3))
            turned[f, 2, base : base + HALO, :] = jnp.where(ends, x * present, 0.0)

    def lay_field(f):
        lay(ext.at[f], turned.at[f], line)

    repeat(FIELDS, lay_field)
    for v in range(V):
        for j in range(3):
            c = ext[COEF, j, vec(v), :]
            r = 1.0 / (1.0 + 4.0 * c)
            inv[j, vec(v), :] = r
            cof[j, vec(v), :] = c * r
            rhs[0, j, vec(v), :] = ext[MID, j, vec(v), :] + ext[4, j, vec(v), :]
            rhs[1, j, vec(v), :] = ext[0, j, vec(v), :]
            rhs[2, j, vec(v), :] = ext[LAST, j, vec(v), :]
    put_edges(edges[0], rhs, range(3))

    def forced_step(k):
        def add(f, j, v, u):
            return u if f == 2 else u + ext[(5 if f == 0 else 1) + k, j, vec(v), :]

        step(rhs, mid, scaled, inv, cof, range(3), 3, V, add, edges)

    repeat(FACTOR - 1, forced_step)

    def between():
        for v in range(V):
            for j in range(3):
                new, old = rhs[0, j, vec(v), :], ext[LAST, j, vec(v), :]
                moved = not_end * (new - old)
                own_new[j, vec(v), :] = new
                scaled[0, j, vec(v), :] = old + moved
                rhs[0, j, vec(v), :] = moved
                s = rhs[1, j, vec(v), :]
                forced[j, vec(v), :] = s
                rhs[1, j, vec(v), :] = s - ext[MID, j, vec(v), :]
        put_edges(edges[0], rhs, range(2))
        squeeze(main, scaled.at[0])
        for j in range(2):
            cols = slice(128 * j, 128 * j + 128)
            at = PART1 + 2 * HALO * j
            main[at : at + HALO, :] = above[LAST, :, cols] * x_first
            main[at + HALO : at + 2 * HALO, :] = below[LAST, :, cols] * x_final
        for b in range(3):
            at = PART2 + 2 * HALO * b
            main[at : at + HALO, :] = turned[LAST, b, 0:HALO, :]
            main[at + HALO : at + 2 * HALO, :] = turned[LAST, b, HALO + N : EXT, :]

    def free_step(k):
        step(rhs, mid, scaled, inv, cof, range(3), 3, V, keep, edges)
        pl.when(k == 0)(between)

    repeat(FACTOR + 1, free_step)
    for k, (ref, f) in enumerate(((rhs, 1), (rhs, 0), (rhs, 2), (ext, COEF))):
        pair[:, 0:128] = restrict(ref, f, pair)
        unmix(rows_c, lambda v: pair[vec(v), 0:128], HV)
        coarse[k] = rows_c[8 : 8 + C, :]
    for k in range(4):
        up[k] = coarse[k, 0:HALO, :]
        down[k] = coarse[k, C - HALO : C, :]
    lo, hi = pack_edges([(coarse[k], coarse[k]) for k in range(4)], C)
    low_c[...] = lo[0]
    high_c[...] = hi[0]


def coarse_edges_body(above, below, low_c, high_c, low, high):
    place, ends = lax.axis_index("sx"), lax.axis_size("sx") - 1
    low[HALO : HALO + C, :] = low_c[...]
    high[HALO : HALO + C, :] = high_c[...]
    for ref, base, present in ((above, 0, flag(place > 0)), (below, HALO + C, flag(place < ends))):
        lo, hi = pack_edges([(ref[k] * present,) * 2 for k in range(4)], HALO)
        low[base : base + HALO, :] = lo[0]
        high[base : base + HALO, :] = hi[0]


ONE = 2 * CEXT + CEXT // 4
TWO = CEXT + CEXT // 5


def coarse_body(coarse, above, below, before, after, one, two, three, four, coefs, ext, rhs, mid, scaled, wide):
    t, x, z = lax.axis_index("tm"), lax.axis_index("sx"), lax.axis_index("sy")
    not_end = flag(t < lax.axis_size("tm") - 1)
    x_first, x_final = flag(x > 0), flag(x < lax.axis_size("sx") - 1)
    z_first, z_final = flag(z > 0), flag(z < lax.axis_size("sy") - 1)
    for k in range(4):
        wide[0:HALO, :] = above[k] * x_first
        wide[HALO : HALO + C, :] = coarse[k]
        wide[HALO + C : CEXT, :] = below[k] * x_final
        mix(ext.at[k, 0], natural(wide, CV), CV)
    for v in range(CV):
        left, right = natural(before, CV)(v), natural(after, CV)(v)
        for k in range(4):
            ext[k, 1, vec(v), :] = side_column(left, right, k, 8, z_first, z_final)
    inv, cof = coefs.at[0], coefs.at[1]
    for j in range(2):
        c = ext[3, j]
        r = 1.0 / (1.0 + 4.0 * c)
        inv[j] = r
        cof[j] = c * r
        rhs[0, j] = ext[0, j] * not_end
        rhs[1, j] = ext[1, j]

    def advance(fields, after_step):
        step(rhs, mid, scaled, inv, cof, fields, 2, CV, after_step)

    def reader(ref, f):
        return lambda r, n: ref[f, 1, r : r + n, :]

    one[0:CEXT, :] = ext[0, 0]
    one[CEXT : 2 * CEXT, :] = ext[1, 0]
    fold(one, 2 * CEXT, [reader(ext, 0), reader(ext, 1)], 8, 4, CEXT)
    advance(range(2), lambda f, j, v, u: u if f == 0 else u + ext[2, j, vec(v), :])
    for j in range(2):
        ext[2, j] = rhs[1, j]
    advance(range(2), lambda f, j, v, u: u + ext[2, j, vec(v), :] if f == 0 else u)
    two[0:CEXT, :] = rhs[0, 0]
    fold(two, CEXT, [reader(rhs, 0)], 8, 5, CEXT)
    repeat(2, lambda k: advance(range(2), keep))
    three[0:CEXT, :] = rhs[0, 0]
    fold(three, CEXT, [reader(rhs, 0)], 8, 5, CEXT)
    advance(range(1, 2), keep)
    for j in range(2):
        four[j] = rhs[1, j]


def arrive_body(
    last, main, ext, coefs, forced, resid, new_start, new_mid, coarse_mid,
    rhs, mid, scaled, turned, top, bottom, edge, line, pair,
):
    inv, cof = coefs.at[0], coefs.at[1]
    edge[...] = jnp.zeros((128, 128), F32)
    for j in range(2):
        at, cols = PART1 + 2 * HALO * j, slice(128 * j, 128 * j + 128)
        top[:, cols] = main[at : at + HALO, :]
        bottom[:, cols] = main[at + HALO : at + 2 * HALO, :]
    for b in range(3):
        at = PART2 + 2 * HALO * b
        turned[b, 0:HALO, :] = main[at : at + HALO, :]
        turned[b, HALO + N : EXT, :] = main[at + HALO : at + 2 * HALO, :]
    turn(turned, last)
    turn_edge(turned, top, bottom, edge)
    lay(rhs.at[0], turned, line)
    unsqueeze(new_start, main)
    for j in range(3):
        rhs[1, j] = new_start[j] - rhs[0, j]
    repeat(FACTOR, lambda k: step(rhs, mid, scaled, inv, cof, range(2), 3, V, keep))
    for j in range(3):
        for v in range(V):
            u = rhs[0, j, vec(v), :] + forced[j, vec(v), :]
            new_mid[j, vec(v), :] = u
            rhs[0, j, vec(v), :] = u - ext[MID, j, vec(v), :]
    repeat(FACTOR, lambda k: step(rhs, mid, scaled, inv, cof, range(1), 3, V, keep))
    for k in range(2):

        def put(b, h, block, k=k):
            resid[k, 128 * b : 128 * b + 128, 128 * h : 128 * h + 128] = block

        unlay(put, lambda j, v, k=k: rhs[1 - k, j, vec(v), :], line, turned)
    coarse_mid[...] = restrict(rhs, 0, pair)


def final_body(
    one, two, three, four, ccoefs, coarse_mid, ext, coefs, new_start, new_mid, own_new,
    out, err, cmid, cscaled, sent, fix, rhs, mid, scaled, turned, line, pair, rows_c, stage, sems,
):
    t = lax.axis_index("tm")
    m1, m2, m3 = flag(t > 0), flag(t > 1), flag(t > 2)
    inv, cof = ccoefs.at[0], ccoefs.at[1]

    def put(k):
        def write(r, n, value):
            sent[k, r : r + n, :] = value

        return write

    unfold(one, 2 * CEXT, 0, 2, 8, 4, CEXT, put(0))
    unfold(one, 2 * CEXT, 1, 2, 8, 4, CEXT, put(1))
    unfold(two, CEXT, 0, 1, 8, 5, CEXT, put(2))
    unfold(three, CEXT, 0, 1, 8, 5, CEXT, put(3))
    err[0, 0] = m1 * (one[0:CEXT, :] + two[0:CEXT, :]) + m2 * three[0:CEXT, :] + m3 * four[0]
    err[0, 1] = m1 * (sent[0] + sent[2]) + m2 * sent[3] + m3 * four[1]

    def spread(k, extra=None):
        src = lax.broadcasted_iota(jnp.int32, (256, 384), 0)
        dst = lax.broadcasted_iota(jnp.int32, (256, 384), 1)
        cell = (3 * (dst % 128) + dst // 128) // 2 - 8
        cell = jnp.where(cell < 0, cell + 2 * C, jnp.where(dst % 128 < LIVE, cell, -1))
        pick = flag(src == cell).astype(jnp.bfloat16)
        for c in range(2):
            unmix(rows_c, lambda v: err[0, c, vec(v), :], CV)
            for v in range(HV):
                pair[vec(v), 128 * c : 128 * c + 128] = natural(rows_c, HV, 8)(v)
        if extra is not None:
            pair[:, 0:128] += extra[...]
        got = select(pair[...], pick)
        for j in range(3):
            fix[k, j] = got[:, 128 * j : 128 * j + 128]

    spread(0)
    step(err, cmid, cscaled, inv, cof, range(1), 2, CV, keep)
    err[0, 0] += one[CEXT : 2 * CEXT, :]
    err[0, 1] += sent[1]
    spread(1)
    step(err, cmid, cscaled, inv, cof, range(1), 2, CV, keep)
    spread(2, coarse_mid)
    inv, cof = coefs.at[0], coefs.at[1]
    for v in range(V):
        for j in range(3):
            rhs[0, j, vec(v), :] = new_start[j, vec(v), :] + fix[0, j, vec(v // 2), :] + ext[0, j, vec(v), :]
            u = new_mid[j, vec(v), :] + fix[1, j, vec(v // 2), :]
            scaled[0, j, vec(v), :] = u
            rhs[1, j, vec(v), :] = u + ext[4, j, vec(v), :]
            scaled[1, j, vec(v), :] = own_new[j, vec(v), :] + fix[2, j, vec(v // 2), :]

    def send(f, at):
        return pltpu.make_async_copy(stage.at[4 * f + at], out.at[4 * f + at], sems.at[4 * f + at])

    def give(at):
        for f in range(2):

            def put(b, h, block, f=f):
                stage[4 * f + at, 128 * b : 128 * b + 128, 128 * h : 128 * h + 128] = block

            unlay(put, lambda j, v, f=f: scaled[f, j, vec(v), :], line, turned)
            send(f, at).start()

    give(FACTOR - 1)

    def fine(k):
        def add(f, j, v, u):
            scaled[f, j, vec(v), :] = u
            return u + ext[4 * f + 1 + k, j, vec(v), :]

        step(rhs, mid, scaled, inv, cof, range(2), 3, V, add)
        give(k)

    repeat(FACTOR - 1, fine)
    for f in range(2):
        for at in range(FACTOR):
            send(f, at).wait()


def ring(x, axis, by):
    count = lax.axis_size(axis)
    return lax.ppermute(x, axis, [(i, (i + by) % count) for i in range(count)])


def vmem(*shape):
    return pltpu.VMEM(shape, F32)


def shards(iterate, source, start_field, conduct):
    up, down, src, middle, last, coef = call(
        load_body, [(FIELDS, HALO, N)] * 2 + [(8, N, N)] + [(N, N)] * 3, [HB] * 4, [pltpu.SemaphoreType.DMA((4,))],
        limit=52_000_000,
    )(source, iterate, start_field, conduct)
    above, below = ring(down, "sx", 1), ring(up, "sx", -1)
    last_in = ring(last, "tm", 1)
    turned, low, high = call(
        center_body, [(FIELDS, 3, EXT, 128), (2, HALO * FIELDS, 128), (2, HALO * FIELDS, 128)], 4, flops=20_000_000
    )(src, middle, last, coef)
    before, after = ring(high, "sy", 1), ring(low, "sy", -1)
    turned, c_lo, c_hi = call(
        rows_body, [(FIELDS, 3, EXT, 128), (3 * HALO, 128), (3 * HALO, 128)], 3,
        [vmem(HALO, N), vmem(HALO, N), vmem(128, 128)], {0: 0},
    )(turned, above, below)
    before_c, after_c = ring(c_hi, "sy", 1), ring(c_lo, "sy", -1)
    _, ext, coefs, forced, own_new, main, c_up, c_down, c_low, c_high, coarse = call(
        local_body,
        [
            (FIELDS, 3, EXT, 128), (FIELDS, 3, EXT, 128), (2, 3, EXT, 128), (3, EXT, 128), (3, EXT, 128), (MAIN, 128),
            (4, HALO, 128), (4, HALO, 128), (C, 128), (C, 128), (4, C, 128),
        ],
        7,
        [vmem(3, 3, EXT, 128)] * 3 + [vmem(EXT, 128), vmem(HALF, 384), vmem(HALF, 128)] + [vmem(3, 2, EXT, 128)] * 2,
        {0: 0}, 50_000_000,
    )(turned, above, below, before, after, before_c, after_c)
    c_above, c_below = ring(c_down, "sx", 1), ring(c_up, "sx", -1)
    main_in = ring(main, "tm", 1)
    c_lo, c_hi = call(coarse_edges_body, [(CEXT, 128)] * 2, 4)(c_above, c_below, c_low, c_high)
    c_before, c_after = ring(c_hi, "sy", 1), ring(c_lo, "sy", -1)
    one, two, three, four, ccoefs = call(
        coarse_body,
        [(ONE, 128), (TWO, 128), (TWO, 128), (2, CEXT, 128), (2, 2, CEXT, 128)],
        5,
        [vmem(4, 2, CEXT, 128)] + [vmem(2, 2, CEXT, 128)] * 3 + [vmem(CEXT, 128)],
    )(coarse, c_above, c_below, c_before, c_after)
    one, two, three = ring(one, "tm", 1), ring(two, "tm", 2), ring(three, "tm", 3)
    resid, new_start, new_mid, coarse_mid = call(
        arrive_body,
        [(2, N, N), (3, EXT, 128), (3, EXT, 128), (HALF, 128)],
        5,
        [vmem(2, 3, EXT, 128)] * 3
        + [vmem(3, EXT, 128), vmem(HALO, N), vmem(HALO, N), vmem(128, 128), vmem(EXT, 128), vmem(HALF, 384)],
        flops=30_000_000,
    )(last_in, main_in, ext, coefs, forced)
    (updated,) = call(
        final_body,
        [(8, N, N)],
        11,
        [vmem(1, 2, CEXT, 128)] * 3 + [vmem(4, CEXT, 128), vmem(3, 3, HALF, 128)] + [vmem(2, 3, EXT, 128)] * 3
        + [vmem(2, EXT, 128), vmem(EXT, 128), vmem(HALF, 256), vmem(CEXT, 128), vmem(8, N, N)]
        + [pltpu.SemaphoreType.DMA((8,))],
        out_specs=[HB],
    )(one, two, three, four, ccoefs, coarse_mid, ext, coefs, new_start, new_mid, own_new)
    return updated, resid


def solution(mesh):
    in_specs = (P("tm", "sx", "sy"), P("tm", "sx", "sy"), P("sx", "sy"), P("sx", "sy"))
    out_specs = (P("tm", "sx", "sy"), P("tm", "sx", "sy"))
    return jax.shard_map(shards, mesh=mesh, in_specs=in_specs, out_specs=out_specs, check_vma=False)
```

```python
import jax
import jax.numpy as jnp
from jax import lax
from jax.experimental import pallas as pl
from jax.experimental.pallas import tpu as pltpu
from jax.sharding import PartitionSpec as P


FACTOR = 4
N = 256
HALO = 16
EXT = N + 2 * HALO
V = EXT // 8
C = N // 2
CEXT = C + 2 * HALO
CV = CEXT // 8
HALF = EXT // 2
HV = HALF // 8
FIELDS = 11
MID, LAST, COEF = 8, 9, 10
LIVE = EXT // 3
F32 = jnp.float32
LIMIT = 24 * 1024 * 1024

VM = pl.BlockSpec(memory_space=pltpu.VMEM)
HB = pl.BlockSpec(memory_space=pltpu.HBM)


def call(body, outs, ins, scratch=(), aliases=None, flops=0, limit=LIMIT, out_specs=None):
    return pl.pallas_call(
        body,
        out_shape=[jax.ShapeDtypeStruct(s, F32) for s in outs],
        in_specs=[VM] * ins if isinstance(ins, int) else ins,
        out_specs=out_specs or [VM] * len(outs),
        scratch_shapes=list(scratch),
        input_output_aliases=aliases or {},
        compiler_params=pltpu.CompilerParams(vmem_limit_bytes=limit),
        cost_estimate=pl.CostEstimate(flops=flops, bytes_accessed=1000, transcendentals=0),
    )


def lanes(rows):
    return lax.broadcasted_iota(jnp.int32, (rows, 128), 1)


def roll(x, by):
    by %= 128
    return pltpu.roll(x, by, 1) if by else x


def flag(condition):
    return jnp.where(condition, 1.0, 0.0).astype(F32)


def vec(v):
    return slice(8 * v, 8 * v + 8)


def mix(dest, read, count):
    for v in range(count):
        dest[vec(v), :] = read(v)


def natural(ref, count, offset=0):
    return lambda v: ref[pl.ds(offset + v, 8, stride=count), :]


def unmix(dest, read, count):
    for v in range(count):
        dest[pl.ds(v, 8, stride=count), :] = read(v)


def sweep(src, edge, fields, cols, count, emit):
    lane = lanes(8)
    first, last = lane == 0, lane == 127
    held = {}

    def at(f, j, v):
        if (f, j, v) not in held:
            held[f, j, v] = src[f, j, vec(v), :]
        return held[f, j, v]

    for v in range(count):
        for f in fields:
            mid = [at(f, j, v) for j in range(cols)]
            if cols == 3:
                ends = None if edge is None else (edge[f, 0, vec(v), :], edge[f, 1, vec(v), :])
                ends = ends or (pltpu.roll(mid[2], 1, 1), pltpu.roll(mid[0], 127, 1))
                left, right = [ends[0], mid[0], mid[1]], [mid[1], mid[2], ends[1]]
            else:
                back = [pltpu.roll(m, 1, 1) for m in mid]
                ahead = [pltpu.roll(m, 127, 1) for m in mid]
                left = [jnp.where(first, back[1 - j], back[j]) for j in range(2)]
                right = [jnp.where(last, ahead[1 - j], ahead[j]) for j in range(2)]
            for j in range(cols):
                below = at(f, j, v + 1) if v + 1 < count else pltpu.roll(src[f, j, vec(0), :], 7, 0)
                above = at(f, j, v - 1) if v else pltpu.roll(src[f, j, vec(count - 1), :], 1, 0)
                emit(f, j, v, mid[j], (below + above) + (left[j] + right[j]))
        for key in [k for k in held if k[2] < v]:
            del held[key]


def put_edge(edge, f, j, v, x):
    if edge is not None and j == 2:
        edge[f, 0, vec(v), :] = pltpu.roll(x, 1, 1)
    if edge is not None and j == 0:
        edge[f, 1, vec(v), :] = pltpu.roll(x, 127, 1)


def step(rhs, mid, scaled, inv, cof, fields, cols, count, after, edges=(None, None)):
    def one(f, j, v, own, total):
        b = own * inv[j, vec(v), :]
        scaled[f, j, vec(v), :] = b
        w = b + cof[j, vec(v), :] * total
        mid[f, j, vec(v), :] = w
        put_edge(edges[1], f, j, v, w)

    def two(f, j, v, own, total):
        u = scaled[f, j, vec(v), :] + cof[j, vec(v), :] * total
        b = after(f, j, v, u)
        rhs[f, j, vec(v), :] = b
        put_edge(edges[0], f, j, v, b)

    sweep(rhs, edges[0], fields, cols, count, one)
    sweep(mid, edges[1], fields, cols, count, two)


def put_edges(edge, rhs, fields):
    for f in fields:
        for v in range(V):
            for j in (0, 2):
                put_edge(edge, f, j, v, rhs[f, j, vec(v), :])


def keep(f, j, v, u):
    return u


def repeat(count, body):
    def one(k, carry):
        body(k)
        return carry

    lax.fori_loop(0, count, one, 0)


def turn(dst, ref):
    for h in range(2):
        for b in range(2):
            block = ref[128 * b : 128 * b + 128, 128 * h : 128 * h + 128]
            dst[b, HALO + 128 * h : HALO + 128 * h + 128, :] = block.T


def turn_edge(dst, above, below, edge):
    for h in range(2):
        cols = slice(128 * h, 128 * h + 128)
        edge[0:HALO, :] = below[:, cols]
        edge[128 - HALO : 128, :] = above[:, cols]
        dst[2, HALO + 128 * h : HALO + 128 * h + 128, :] = edge[...].T


def lay(dst, turned, line):
    pad = jnp.zeros((128 - LIVE, 128), F32)
    for j in range(3):
        for b in range(3):
            got = jnp.concatenate([turned[b, pl.ds(j, LIVE, stride=3), :], pad], axis=0).T
            if b < 2:
                line[j, HALO + 128 * b : HALO + 128 * b + 128, :] = got
            else:
                line[j, HALO + N : EXT, :] = got[0:HALO, :]
                line[j, 0:HALO, :] = got[128 - HALO : 128, :]
    for j in range(3):
        mix(dst.at[j], natural(line.at[j], V), V)


def unlay(write, read, line, turned):
    for j in range(3):
        unmix(line.at[j], lambda v: read(j, v), V)
        for b in range(2):
            got = line[j, HALO + 128 * b : HALO + 128 * b + 128, :].T
            turned[b, pl.ds(j, LIVE, stride=3), :] = got[0:LIVE, :]
    for b in range(2):
        for h in range(2):
            write(b, h, turned[b, HALO + 128 * h : HALO + 128 * h + 128, :].T)


def select(x, pick):
    high = x.astype(jnp.bfloat16)
    rest = x - high.astype(F32)
    mid = rest.astype(jnp.bfloat16)
    low = (rest - mid.astype(F32)).astype(jnp.bfloat16)
    parts = [jnp.dot(p, pick, preferred_element_type=F32) for p in (low, mid, high)]
    return (parts[0] + parts[1]) + parts[2]


def restrict(ref, f, pair):
    lane = lax.broadcasted_iota(jnp.int32, (3 * 128, C), 0)
    coarse = lax.broadcasted_iota(jnp.int32, (3 * 128, C), 1)
    column = 3 * (lane % 128) + lane // 128
    pick = jnp.where(column // 2 - 8 == coarse, 0.25, 0.0).astype(jnp.bfloat16)
    for j in range(3):
        for i in range(HV):
            pair[vec(i), 128 * j : 128 * j + 128] = ref[f, j, vec(2 * i), :] + ref[f, j, vec(2 * i + 1), :]
    return select(pair[...], pick)


def load_body(source, iterate, start, conduct, up, down, src, middle, last, coef, sems):
    is_end = lax.axis_index("tm") == lax.axis_size("tm") - 1
    pairs = ((source, src), (iterate.at[3], middle), (conduct, coef))
    copies = [pltpu.make_async_copy(a, b, sems.at[i]) for i, (a, b) in enumerate(pairs)]
    for c in copies:
        c.start()

    @pl.when(is_end)
    def _():
        c = pltpu.make_async_copy(start, last, sems.at[3])
        c.start()
        c.wait()

    @pl.when(jnp.logical_not(is_end))
    def _():
        c = pltpu.make_async_copy(iterate.at[7], last, sems.at[3])
        c.start()
        c.wait()

    for c in copies:
        c.wait()
    for f, ref in enumerate([src.at[f] for f in range(8)] + [middle, last, coef]):
        up[f] = ref[0:HALO, :]
        down[f] = ref[N - HALO : N, :]


def pack_edges(pieces, rows):
    lane = lanes(rows)
    low = [jnp.zeros((rows, 128), F32) for _ in range((len(pieces) + 7) // 8)]
    high = list(low)
    for f, (head, tail) in enumerate(pieces):
        at, k = HALO * (f % 8), f // 8
        inside = (lane >= at) & (lane < at + HALO)
        low[k] = jnp.where(inside, roll(head, at), low[k])
        high[k] = jnp.where(inside, roll(tail, at + HALO), high[k])
    return low, high


def center_body(src, middle, last, coef, turned, low, high):
    for f, ref in enumerate([src.at[f] for f in range(8)] + [middle, last, coef]):
        turn(turned.at[f], ref)
        for b in range(2):
            at = slice(HALO * f, HALO * f + HALO)
            low[b, at, :] = turned[f, b, HALO : 2 * HALO, :]
            high[b, at, :] = turned[f, b, N : N + HALO, :]


def rows_body(turned_in, above, below, turned, low, high, top, bottom, edge):
    del turned_in
    place, ends = lax.axis_index("sx"), lax.axis_size("sx") - 1
    up, down = flag(place > 0), flag(place < ends)
    edge[...] = jnp.zeros((128, 128), F32)
    lane = lanes(HALO)
    out = {}
    for f in range(FIELDS):
        top[...] = above[f] * up
        bottom[...] = below[f] * down
        turn_edge(turned.at[f], top, bottom, edge)
        at = 2 * HALO * (f // 3)
        for k, base in ((0, HALO), (1, N)):
            x = roll(turned[f, 2, base : base + HALO, :], HALO + at)
            old = out.get((k, f % 3), jnp.zeros((HALO, 128), F32))
            out[k, f % 3] = jnp.where((lane >= at) & (lane < at + 2 * HALO), x, old)
    for i in range(3):
        low[HALO * i : HALO * i + HALO, :] = out[0, i]
        high[HALO * i : HALO * i + HALO, :] = out[1, i]


def side_column(before, after, f, rows, first, final):
    lane = lanes(rows)
    at = HALO * (f % 8)
    right = jnp.where(lane < HALO, roll(after, -at) * final, 0.0)
    return jnp.where(lane >= 128 - HALO, roll(before, -HALO - at) * first, right)


QUARTER = EXT // 4
PART1 = 2 * EXT + QUARTER
PART2 = PART1 + 4 * HALO
MAIN = PART2 + 6 * HALO


def squeeze(dest, ref):
    lane = lanes(8)
    for v in range(V):
        third = ref[2, vec(v), :]
        dest[8 * v : 8 * v + 8, :] = jnp.where(lane < LIVE, ref[0, vec(v), :], roll(third, 96))
        dest[EXT + 8 * v : EXT + 8 * v + 8, :] = jnp.where(lane < LIVE, ref[1, vec(v), :], roll(third, 64))
    for i in range(QUARTER // 8):
        out = None
        for g in range(4):
            x = roll(ref[2, vec(i + g * QUARTER // 8), :], 32 * g - 64)
            out = x if out is None else jnp.where(lane >= 32 * g, x, out)
        dest[2 * EXT + 8 * i : 2 * EXT + 8 * i + 8, :] = out


def unsqueeze(dest, src):
    lane = lanes(8)
    for v in range(V):
        a, b = src[8 * v : 8 * v + 8, :], src[EXT + 8 * v : EXT + 8 * v + 8, :]
        dest[0, vec(v), :] = jnp.where(lane < LIVE, a, 0.0)
        dest[1, vec(v), :] = jnp.where(lane < LIVE, b, 0.0)
        g, i = divmod(v, QUARTER // 8)
        rest = roll(src[2 * EXT + 8 * i : 2 * EXT + 8 * i + 8, :], 64 - 32 * g)
        third = jnp.where(lane < 32, roll(a, 32), jnp.where(lane < 64, roll(b, 64), rest))
        dest[2, vec(v), :] = jnp.where(lane < LIVE, third, 0.0)


def fold(dest, base, columns, width, groups, rows_in):
    span = 2 * width
    rows = rows_in // groups
    lane = lanes(rows)
    out = jnp.zeros((rows, 128), F32)
    for g in range(groups):
        for k, read in enumerate(columns):
            at = (g * len(columns) + k) * span
            inside = (lane >= at) & (lane < at + span)
            out = jnp.where(inside, roll(read(g * rows, rows), width + at), out)
    dest[base : base + rows, :] = out


def unfold(src, base, k, count, width, groups, rows_in, write):
    span = 2 * width
    rows = rows_in // groups
    lane = lanes(rows)
    for g in range(groups):
        at = (g * count + k) * span
        x = roll(src[base : base + rows, :], -width - at)
        write(g * rows, rows, jnp.where((lane < width) | (lane >= 128 - width), x, 0.0))


def local_body(
    turned_in, above, below, before, after, before_c, after_c,
    turned, ext, coefs, forced, own_new, main, up, down, low_c, high_c, coarse,
    rhs, mid, scaled, line, pair, rows_c, *edges,
):
    del turned_in
    t, x, z = lax.axis_index("tm"), lax.axis_index("sx"), lax.axis_index("sy")
    not_end = flag(t < lax.axis_size("tm") - 1)
    x_first, x_final = flag(x > 0), flag(x < lax.axis_size("sx") - 1)
    z_first, z_final = flag(z > 0), flag(z < lax.axis_size("sy") - 1)
    inv, cof = coefs.at[0], coefs.at[1]
    lane = lanes(HALO)
    ends = (lane < HALO) | (lane >= 128 - HALO)
    for f in range(FIELDS):
        for own, corner, base, present in ((before, before_c, 0, z_first), (after, after_c, HALO + N, z_final)):
            for b in range(2):
                turned[f, b, base : base + HALO, :] = own[b, HALO * f : HALO * f + HALO, :] * present
            x = roll(corner[HALO * (f % 3) : HALO * (f % 3) + HALO, :], -HALO - 2 * HALO * (f // 3))
            turned[f, 2, base : base + HALO, :] = jnp.where(ends, x * present, 0.0)

    def lay_fields(k):
        for i in range(2):
            lay(ext.at[2 * k + i], turned.at[2 * k + i], line.at[i])

    repeat(FIELDS // 2, lay_fields)
    lay(ext.at[FIELDS - 1], turned.at[FIELDS - 1], line.at[0])
    for v in range(V):
        for j in range(3):
            c = ext[COEF, j, vec(v), :]
            r = 1.0 / (1.0 + 4.0 * c)
            inv[j, vec(v), :] = r
            cof[j, vec(v), :] = c * r
            rhs[0, j, vec(v), :] = ext[MID, j, vec(v), :] + ext[4, j, vec(v), :]
            rhs[1, j, vec(v), :] = ext[0, j, vec(v), :]
            rhs[2, j, vec(v), :] = ext[LAST, j, vec(v), :]
    put_edges(edges[0], rhs, range(3))

    def forced_step(k):
        def add(f, j, v, u):
            return u if f == 2 else u + ext[(5 if f == 0 else 1) + k, j, vec(v), :]

        step(rhs, mid, scaled, inv, cof, range(3), 3, V, add, edges)

    repeat(FACTOR - 1, forced_step)

    def between():
        for v in range(V):
            for j in range(3):
                new, old = rhs[0, j, vec(v), :], ext[LAST, j, vec(v), :]
                moved = not_end * (new - old)
                own_new[j, vec(v), :] = new
                scaled[0, j, vec(v), :] = old + moved
                rhs[0, j, vec(v), :] = moved
                s = rhs[1, j, vec(v), :]
                forced[j, vec(v), :] = s
                rhs[1, j, vec(v), :] = s - ext[MID, j, vec(v), :]
        put_edges(edges[0], rhs, range(2))
        squeeze(main, scaled.at[0])
        for j in range(2):
            cols = slice(128 * j, 128 * j + 128)
            at = PART1 + 2 * HALO * j
            main[at : at + HALO, :] = above[LAST, :, cols] * x_first
            main[at + HALO : at + 2 * HALO, :] = below[LAST, :, cols] * x_final
        for b in range(3):
            at = PART2 + 2 * HALO * b
            main[at : at + HALO, :] = turned[LAST, b, 0:HALO, :]
            main[at + HALO : at + 2 * HALO, :] = turned[LAST, b, HALO + N : EXT, :]

    def free_step(k):
        step(rhs, mid, scaled, inv, cof, range(3), 3, V, keep, edges)
        pl.when(k == 0)(between)

    repeat(FACTOR + 1, free_step)
    for k, (ref, f) in enumerate(((rhs, 1), (rhs, 0), (rhs, 2), (ext, COEF))):
        got = restrict(ref, f, pair.at[k])
        unmix(rows_c.at[k], lambda v: got[vec(v), :], HV)
        coarse[k] = rows_c[k, 8 : 8 + C, :]
    for k in range(4):
        up[k] = coarse[k, 0:HALO, :]
        down[k] = coarse[k, C - HALO : C, :]
    lo, hi = pack_edges([(coarse[k], coarse[k]) for k in range(4)], C)
    low_c[...] = lo[0]
    high_c[...] = hi[0]


def coarse_edges_body(above, below, low_c, high_c, low, high):
    place, ends = lax.axis_index("sx"), lax.axis_size("sx") - 1
    low[HALO : HALO + C, :] = low_c[...]
    high[HALO : HALO + C, :] = high_c[...]
    for ref, base, present in ((above, 0, flag(place > 0)), (below, HALO + C, flag(place < ends))):
        lo, hi = pack_edges([(ref[k] * present,) * 2 for k in range(4)], HALO)
        low[base : base + HALO, :] = lo[0]
        high[base : base + HALO, :] = hi[0]


ONE = 2 * CEXT + CEXT // 4
TWO = CEXT + CEXT // 5


def coarse_body(coarse, above, below, before, after, one, two, three, four, coefs, ext, rhs, mid, scaled, wide):
    t, x, z = lax.axis_index("tm"), lax.axis_index("sx"), lax.axis_index("sy")
    not_end = flag(t < lax.axis_size("tm") - 1)
    x_first, x_final = flag(x > 0), flag(x < lax.axis_size("sx") - 1)
    z_first, z_final = flag(z > 0), flag(z < lax.axis_size("sy") - 1)
    for k in range(4):
        wide[0:HALO, :] = above[k] * x_first
        wide[HALO : HALO + C, :] = coarse[k]
        wide[HALO + C : CEXT, :] = below[k] * x_final
        mix(ext.at[k, 0], natural(wide, CV), CV)
    for v in range(CV):
        left, right = natural(before, CV)(v), natural(after, CV)(v)
        for k in range(4):
            ext[k, 1, vec(v), :] = side_column(left, right, k, 8, z_first, z_final)
    inv, cof = coefs.at[0], coefs.at[1]
    for j in range(2):
        c = ext[3, j]
        r = 1.0 / (1.0 + 4.0 * c)
        inv[j] = r
        cof[j] = c * r
        rhs[0, j] = ext[0, j] * not_end
        rhs[1, j] = ext[1, j]

    def advance(fields, after_step):
        step(rhs, mid, scaled, inv, cof, fields, 2, CV, after_step)

    def reader(ref, f):
        return lambda r, n: ref[f, 1, r : r + n, :]

    one[0:CEXT, :] = ext[0, 0]
    one[CEXT : 2 * CEXT, :] = ext[1, 0]
    fold(one, 2 * CEXT, [reader(ext, 0), reader(ext, 1)], 8, 4, CEXT)
    advance(range(2), lambda f, j, v, u: u if f == 0 else u + ext[2, j, vec(v), :])
    for j in range(2):
        ext[2, j] = rhs[1, j]
    advance(range(2), lambda f, j, v, u: u + ext[2, j, vec(v), :] if f == 0 else u)
    two[0:CEXT, :] = rhs[0, 0]
    fold(two, CEXT, [reader(rhs, 0)], 8, 5, CEXT)
    repeat(2, lambda k: advance(range(2), keep))
    three[0:CEXT, :] = rhs[0, 0]
    fold(three, CEXT, [reader(rhs, 0)], 8, 5, CEXT)
    advance(range(1, 2), keep)
    for j in range(2):
        four[j] = rhs[1, j]


def arrive_body(
    last, main, ext, coefs, forced, resid, new_start, new_mid, coarse_mid,
    rhs, mid, scaled, turned, top, bottom, edge, line, pair,
):
    inv, cof = coefs.at[0], coefs.at[1]
    edge[...] = jnp.zeros((128, 128), F32)
    for j in range(2):
        at, cols = PART1 + 2 * HALO * j, slice(128 * j, 128 * j + 128)
        top[:, cols] = main[at : at + HALO, :]
        bottom[:, cols] = main[at + HALO : at + 2 * HALO, :]
    for b in range(3):
        at = PART2 + 2 * HALO * b
        turned[b, 0:HALO, :] = main[at : at + HALO, :]
        turned[b, HALO + N : EXT, :] = main[at + HALO : at + 2 * HALO, :]
    turn(turned, last)
    turn_edge(turned, top, bottom, edge)
    lay(rhs.at[0], turned, line)
    unsqueeze(new_start, main)
    for j in range(3):
        rhs[1, j] = new_start[j] - rhs[0, j]
    repeat(FACTOR, lambda k: step(rhs, mid, scaled, inv, cof, range(2), 3, V, keep))
    for j in range(3):
        for v in range(V):
            u = rhs[0, j, vec(v), :] + forced[j, vec(v), :]
            new_mid[j, vec(v), :] = u
            rhs[0, j, vec(v), :] = u - ext[MID, j, vec(v), :]
    repeat(FACTOR, lambda k: step(rhs, mid, scaled, inv, cof, range(1), 3, V, keep))
    for k in range(2):

        def put(b, h, block, k=k):
            resid[k, 128 * b : 128 * b + 128, 128 * h : 128 * h + 128] = block

        unlay(put, lambda j, v, k=k: rhs[1 - k, j, vec(v), :], line, turned)
    coarse_mid[...] = restrict(rhs, 0, pair)


def final_body(
    one, two, three, four, ccoefs, coarse_mid, ext, coefs, new_start, new_mid, own_new,
    out, err, cmid, cscaled, sent, fix, rhs, mid, scaled, turned, line, pair, rows_c, stage, sems,
):
    t = lax.axis_index("tm")
    m1, m2, m3 = flag(t > 0), flag(t > 1), flag(t > 2)
    inv, cof = ccoefs.at[0], ccoefs.at[1]

    def put(k):
        def write(r, n, value):
            sent[k, r : r + n, :] = value

        return write

    unfold(one, 2 * CEXT, 0, 2, 8, 4, CEXT, put(0))
    unfold(one, 2 * CEXT, 1, 2, 8, 4, CEXT, put(1))
    unfold(two, CEXT, 0, 1, 8, 5, CEXT, put(2))
    unfold(three, CEXT, 0, 1, 8, 5, CEXT, put(3))
    err[0, 0] = m1 * (one[0:CEXT, :] + two[0:CEXT, :]) + m2 * three[0:CEXT, :] + m3 * four[0]
    err[0, 1] = m1 * (sent[0] + sent[2]) + m2 * sent[3] + m3 * four[1]

    def spread(k, extra=None):
        src = lax.broadcasted_iota(jnp.int32, (256, 384), 0)
        dst = lax.broadcasted_iota(jnp.int32, (256, 384), 1)
        cell = (3 * (dst % 128) + dst // 128) // 2 - 8
        cell = jnp.where(cell < 0, cell + 2 * C, jnp.where(dst % 128 < LIVE, cell, -1))
        pick = flag(src == cell).astype(jnp.bfloat16)
        for c in range(2):
            unmix(rows_c, lambda v: err[0, c, vec(v), :], CV)
            for v in range(HV):
                pair[vec(v), 128 * c : 128 * c + 128] = natural(rows_c, HV, 8)(v)
        if extra is not None:
            pair[:, 0:128] += extra[...]
        got = select(pair[...], pick)
        for j in range(3):
            fix[k, j] = got[:, 128 * j : 128 * j + 128]

    spread(0)
    step(err, cmid, cscaled, inv, cof, range(1), 2, CV, keep)
    err[0, 0] += one[CEXT : 2 * CEXT, :]
    err[0, 1] += sent[1]
    spread(1)
    step(err, cmid, cscaled, inv, cof, range(1), 2, CV, keep)
    spread(2, coarse_mid)
    inv, cof = coefs.at[0], coefs.at[1]
    for v in range(V):
        for j in range(3):
            rhs[0, j, vec(v), :] = new_start[j, vec(v), :] + fix[0, j, vec(v // 2), :] + ext[0, j, vec(v), :]
            u = new_mid[j, vec(v), :] + fix[1, j, vec(v // 2), :]
            scaled[0, j, vec(v), :] = u
            rhs[1, j, vec(v), :] = u + ext[4, j, vec(v), :]
            scaled[1, j, vec(v), :] = own_new[j, vec(v), :] + fix[2, j, vec(v // 2), :]

    def send(f, at):
        return pltpu.make_async_copy(stage.at[4 * f + at], out.at[4 * f + at], sems.at[4 * f + at])

    def give(at):
        for f in range(2):

            def put(b, h, block, f=f):
                stage[4 * f + at, 128 * b : 128 * b + 128, 128 * h : 128 * h + 128] = block

            unlay(put, lambda j, v, f=f: scaled[f, j, vec(v), :], line.at[f], turned.at[f])
            send(f, at).start()

    give(FACTOR - 1)

    def fine(k):
        def add(f, j, v, u):
            scaled[f, j, vec(v), :] = u
            return u + ext[4 * f + 1 + k, j, vec(v), :]

        step(rhs, mid, scaled, inv, cof, range(2), 3, V, add)
        give(k)

    repeat(FACTOR - 1, fine)
    for f in range(2):
        for at in range(FACTOR):
            send(f, at).wait()


def ring(x, axis, by):
    count = lax.axis_size(axis)
    return lax.ppermute(x, axis, [(i, (i + by) % count) for i in range(count)])


def vmem(*shape):
    return pltpu.VMEM(shape, F32)


def shards(iterate, source, start_field, conduct):
    up, down, src, middle, last, coef = call(
        load_body, [(FIELDS, HALO, N)] * 2 + [(8, N, N)] + [(N, N)] * 3, [HB] * 4, [pltpu.SemaphoreType.DMA((4,))],
        limit=52_000_000,
    )(source, iterate, start_field, conduct)
    above, below = ring(down, "sx", 1), ring(up, "sx", -1)
    last_in = ring(last, "tm", 1)
    turned, low, high = call(
        center_body, [(FIELDS, 3, EXT, 128), (2, HALO * FIELDS, 128), (2, HALO * FIELDS, 128)], 4, flops=20_000_000
    )(src, middle, last, coef)
    before, after = ring(high, "sy", 1), ring(low, "sy", -1)
    turned, c_lo, c_hi = call(
        rows_body, [(FIELDS, 3, EXT, 128), (3 * HALO, 128), (3 * HALO, 128)], 3,
        [vmem(HALO, N), vmem(HALO, N), vmem(128, 128)], {0: 0},
    )(turned, above, below)
    before_c, after_c = ring(c_hi, "sy", 1), ring(c_lo, "sy", -1)
    _, ext, coefs, forced, own_new, main, c_up, c_down, c_low, c_high, coarse = call(
        local_body,
        [
            (FIELDS, 3, EXT, 128), (FIELDS, 3, EXT, 128), (2, 3, EXT, 128), (3, EXT, 128), (3, EXT, 128), (MAIN, 128),
            (4, HALO, 128), (4, HALO, 128), (C, 128), (C, 128), (4, C, 128),
        ],
        7,
        [vmem(3, 3, EXT, 128)] * 3 + [vmem(2, 3, EXT, 128), vmem(4, HALF, 384), vmem(4, HALF, 128)] + [vmem(3, 2, EXT, 128)] * 2,
        {0: 0}, 50_000_000,
    )(turned, above, below, before, after, before_c, after_c)
    c_above, c_below = ring(c_down, "sx", 1), ring(c_up, "sx", -1)
    main_in = ring(main, "tm", 1)
    c_lo, c_hi = call(coarse_edges_body, [(CEXT, 128)] * 2, 4)(c_above, c_below, c_low, c_high)
    c_before, c_after = ring(c_hi, "sy", 1), ring(c_lo, "sy", -1)
    one, two, three, four, ccoefs = call(
        coarse_body,
        [(ONE, 128), (TWO, 128), (TWO, 128), (2, CEXT, 128), (2, 2, CEXT, 128)],
        5,
        [vmem(4, 2, CEXT, 128)] + [vmem(2, 2, CEXT, 128)] * 3 + [vmem(CEXT, 128)],
    )(coarse, c_above, c_below, c_before, c_after)
    one, two, three = ring(one, "tm", 1), ring(two, "tm", 2), ring(three, "tm", 3)
    resid, new_start, new_mid, coarse_mid = call(
        arrive_body,
        [(2, N, N), (3, EXT, 128), (3, EXT, 128), (HALF, 128)],
        5,
        [vmem(2, 3, EXT, 128)] * 3
        + [vmem(3, EXT, 128), vmem(HALO, N), vmem(HALO, N), vmem(128, 128), vmem(3, EXT, 128), vmem(HALF, 384)],
        flops=30_000_000,
    )(last_in, main_in, ext, coefs, forced)
    (updated,) = call(
        final_body,
        [(8, N, N)],
        11,
        [vmem(1, 2, CEXT, 128)] * 3 + [vmem(4, CEXT, 128), vmem(3, 3, HALF, 128)] + [vmem(2, 3, EXT, 128)] * 3
        + [vmem(2, 2, EXT, 128), vmem(2, 3, EXT, 128), vmem(HALF, 256), vmem(CEXT, 128), vmem(8, N, N)]
        + [pltpu.SemaphoreType.DMA((8,))],
        out_specs=[HB],
    )(one, two, three, four, ccoefs, coarse_mid, ext, coefs, new_start, new_mid, own_new)
    return updated, resid


def solution(mesh):
    in_specs = (P("tm", "sx", "sy"), P("tm", "sx", "sy"), P("sx", "sy"), P("sx", "sy"))
    out_specs = (P("tm", "sx", "sy"), P("tm", "sx", "sy"))
    return jax.shard_map(shards, mesh=mesh, in_specs=in_specs, out_specs=out_specs, check_vma=False)
```
